32 devices in a mesh: groups: 1, seq: 32 (over z, y, x, core).
Axes of the slice: x: 2, y: 2, z: 4, core: 2. Of those that a mesh axis runs over, the one named last changes fastest.
Arguments:
- queries: bfloat16 [4096, 4096], P(('groups', 'seq')), may hold values from -100 to 100
- keys_values: bfloat16 [4096, 2, 512], P(('groups', 'seq')), may hold values from -5 to 5
- head_signs: int32 [32, 128], replicated, may hold values from -1 to 1, as said below
- out_codes: int32 [512, 8192], P(None, 'seq'), may hold values from -2147483648 to 2147483647, as said below
- out_scales: bfloat16 [32, 8192], replicated, may hold values from 0.019897461 to 0.19921875
Outputs:
- projected: bfloat16 [4096, 8192], P(('groups', 'seq'))
The draws below stay inside these ranges and needn't reach their ends.
Inputs may be any that keep to these rules, and one draw needn't show every extreme that they name: `head_signs`: every entry is -1 or 1. `out_codes`: each word holds eight codes of 0 to 15, the code of row 8 i + k in bits 4k to 4k + 3 of word row i, the word read as a signed 32-bit integer.
All inputs are finite; a program needn't handle non-finite values.
Results may differ from the reference program's by a relative error of at most 0.006.
Values may be sent and summed in bfloat16 or wider, within the bound.
A program may use at most 128 MiB of HBM per device.

```python
import functools
import math
import jax
import jax.numpy as jnp
from jax import lax

D = 8192
HEADS = 32
KV = 4
HD = 128
GROUP = 128
WINDOW = 2048
TOKENS = 4096


def pair_draw(key):
    query_key = jax.random.fold_in(key, 101)
    kv_key = jax.random.fold_in(key, 102)
    base_queries = jnp.clip(jax.random.normal(query_key, (TOKENS, HEADS * HD), jnp.float32), -4.5, 4.5)
    base_kv = jnp.clip(jax.random.normal(kv_key, (TOKENS, 2, KV * HD), jnp.float32), -4.5, 4.5)
    return (base_queries, base_kv)


def draw_queries(key, part):
    return pair_draw(key)[0].astype(jnp.bfloat16)


def draw_keys_values(key, part):
    return pair_draw(key)[1].astype(jnp.bfloat16)


def draw_head_signs(key, part):
    sign_key = jax.random.fold_in(key, 301)
    return (2 * jax.random.randint(sign_key, (HEADS, HD), 0, 2, jnp.int32) - 1).astype(jnp.int32)


def draw_out_codes(key, part):
    code_key = jax.random.fold_in(key, 401)
    nibbles = jax.random.randint(code_key, (HEADS * HD // 8, D, 8), 0, 16, jnp.int32)
    shifted = [jnp.left_shift(nibbles[:, :, nibble_index], 4 * nibble_index) for nibble_index in range(8)]
    return functools.reduce(jnp.bitwise_or, shifted).astype(jnp.int32)


def setup_inputs(seed: int = 0, part: int = 0) -> dict:
    splits = jax.random.split(jax.random.key(seed), 6)
    part_keys = jax.random.split(jax.random.fold_in(splits[5], part), 6)
    return {
        "queries": draw_queries(jax.random.fold_in(jax.random.fold_in(splits[5], part), 71), part),
        "keys_values": draw_keys_values(jax.random.fold_in(jax.random.fold_in(splits[5], part), 71), part),
        "head_signs": draw_head_signs(jax.random.fold_in(splits[5], 71), part),
        "out_codes": draw_out_codes(jax.random.fold_in(splits[5], 71), part),
        "out_scales": jnp.clip(jnp.exp(jax.random.uniform(splits[4], (HEADS * HD // GROUP, D), jnp.float32, math.log(0.019897461), math.log(0.19921875))), 0.019897461, 0.19921875).astype(jnp.bfloat16),
    }


def hadamard(order):
    index = jnp.arange(order, dtype=jnp.int32)
    common = jnp.bitwise_and(index[:, None], index[None, :])
    ones = jnp.zeros((order, order), jnp.int32)
    for bit_index in range(order.bit_length()):
        ones = ones + jnp.bitwise_and(jnp.right_shift(common, bit_index), 1)
    return jnp.where(ones % 2 == 0, 1.0, -1.0).astype(jnp.float32)

def unpack(code_words):
    nibbles = [jnp.bitwise_and(jnp.right_shift(code_words, 4 * nibble_index), 15) for nibble_index in range(8)]
    stacked = jnp.stack(nibbles, axis=1)
    stacked = stacked.reshape(code_words.shape[0] * 8, code_words.shape[1])
    return (stacked - 8).astype(jnp.float32)

def rotate(attended, head_signs):
    signed = attended * head_signs.astype(jnp.float32)[None]
    mixed = jnp.einsum('thd,de->the', signed, hadamard(HD), precision=lax.Precision.HIGHEST) / math.sqrt(HD)
    return mixed.astype(jnp.bfloat16).reshape(attended.shape[0], HEADS * HD)

def reference(queries, keys_values, head_signs, out_codes, out_scales):
    per_group = HEADS // KV
    block_rows = math.gcd(TOKENS, 512)
    block_count = TOKENS // block_rows
    key_count = WINDOW + block_rows
    padded = jnp.concatenate([jnp.zeros((WINDOW, 2, KV * HD), keys_values.dtype), keys_values], axis=0)

    def attend(block):
        start = (block * block_rows).astype(jnp.int32)
        query_rows = lax.dynamic_slice_in_dim(queries, start, block_rows, 0).astype(jnp.float32)
        query_rows = query_rows.reshape(block_rows, KV, per_group, HD)
        key_value = lax.dynamic_slice_in_dim(padded, start, key_count, 0).astype(jnp.float32)
        key_rows = key_value[:, 0].reshape(key_count, KV, HD)
        value_rows = key_value[:, 1].reshape(key_count, KV, HD)
        scores = jnp.einsum('iGhd,jGd->Ghij', query_rows, key_rows) / math.sqrt(HD)
        query_pos = start + jnp.arange(block_rows, dtype=jnp.int32)
        key_pos = start - WINDOW + jnp.arange(key_count, dtype=jnp.int32)
        distance = query_pos[:, None] - key_pos[None, :]
        allowed = (distance >= 0) & (distance < WINDOW) & (key_pos[None, :] >= 0)
        allowed = allowed[None, None]
        scores = jnp.where(allowed, scores, -jnp.inf)
        row_max = lax.optimization_barrier(jnp.max(scores, axis=-1, keepdims=True))
        weights = jnp.where(allowed, jnp.exp(scores - row_max), 0.0)
        total = lax.optimization_barrier(jnp.sum(weights, axis=-1, keepdims=True))
        rounded = lax.optimization_barrier(weights.astype(jnp.bfloat16)).astype(jnp.float32)
        weighted = jnp.einsum('Ghij,jGd->Ghid', rounded, value_rows) / total
        return jnp.transpose(weighted, (2, 0, 1, 3)).reshape(block_rows, HEADS, HD)
    attended = lax.map(attend, jnp.arange(block_count, dtype=jnp.int32)).reshape(TOKENS, HEADS, HD)
    rotated = rotate(attended, head_signs)
    code_vals = unpack(out_codes)
    scaled = code_vals.reshape(HEADS * HD // GROUP, GROUP, D) * out_scales.astype(jnp.float32)[:, None, :]
    weight = scaled.reshape(HEADS * HD, D).astype(jnp.bfloat16)
    return jnp.dot(rotated, weight, preferred_element_type=jnp.float32).astype(jnp.bfloat16)
```

```python
import functools
import math

import jax
import jax.numpy as jnp
from jax import lax
from jax.experimental import pallas as pl
from jax.experimental.pallas import tpu as pltpu
from jax.sharding import PartitionSpec as P

HEADS = 32
KV = 4
HD = 128
GROUP = 128
WINDOW = 2048
QUAD = 4
LANE_HEADS = HEADS // QUAD
HALVES = 2
PER_STEP = LANE_HEADS // HALVES
STEPS = QUAD * HALVES
LOG2E = 1.4426950408889634
MESH = pl.DeviceIdType.MESH
BF16 = jnp.bfloat16
F32 = jnp.float32


def reordered_hadamard():
    column = jnp.arange(HD, dtype=jnp.int32)
    source = (column % 16) * 8 + column // 16
    common = jnp.bitwise_and(jnp.arange(HD, dtype=jnp.int32)[:, None], source[None, :])
    ones = jnp.zeros((HD, HD), jnp.int32)
    for bit in range(HD.bit_length()):
        ones = ones + jnp.bitwise_and(jnp.right_shift(common, bit), 1)
    return jnp.where(ones % 2 == 0, 1.0, -1.0).astype(BF16)


def kernel(
    n, reach, slots,
    q_ref, kv_ref, sign_ref, had_ref, codes_ref, scales_ref, out_ref,
    win, ones, qbuf, cbuf, rot, bias, stage, local_sem,
    kq_s, kq_r, qs, qr, zs, zr, ys, yr, up_s, up_r, dn_s, dn_r, cy_s, cy_r,
    rx_s, rx_r, rc_s, rc_r, rf_s, rf_r, os, orr, ol,
):
    rows = q_ref.shape[0]
    cols = codes_ref.shape[1]
    planes = n // (2 * QUAD)
    width = LANE_HEADS * HD
    half_width = PER_STEP * HD
    top_slot = slots - 1
    me = lax.axis_index("seq")
    z = me // (2 * QUAD)
    y = (me // QUAD) % 2
    lane = me % QUAD
    quad = me // QUAD
    core, x = lane % 2, lane // 2
    dc, dx, dy = 1 - 2 * core, 2 - 4 * x, QUAD - 2 * QUAD * y
    up, down = me + 2 * QUAD, me - 2 * QUAD
    has_up, has_down = z + 1 < planes, z >= 1

    def off(k):
        return (k % 2) * dc + (k // 2) * dx

    def remote(src, dst, send, recv, target):
        return pltpu.make_async_remote_copy(
            src_ref=src, dst_ref=dst, send_sem=send, recv_sem=recv,
            device_id={"seq": target}, device_id_type=MESH,
        )

    barrier = pltpu.get_barrier_semaphore()

    def greet(target):
        pl.semaphore_signal(barrier, inc=1, device_id={"seq": target}, device_id_type=MESH)

    for k in (2, 3, 1):
        greet(me + off(k))
    greet(me + dy)

    @pl.when(has_up)
    def _():
        greet(up)

    @pl.when(has_down)
    def _():
        greet(down)

    own_kv = pltpu.make_async_copy(
        kv_ref.at[lane], win.at[top_slot * QUAD + lane, :, pl.ds(0, 2 * HD)], local_sem.at[0])
    own_lanes = pl.ds(pl.multiple_of(lane * width, width), width)
    own_q = pltpu.make_async_copy(q_ref.at[:, own_lanes], qbuf.at[0], local_sem.at[1])
    own_codes = pltpu.make_async_copy(codes_ref, cbuf.at[quad], local_sem.at[2])
    own_kv.start()
    own_q.start()
    own_codes.start()

    pl.semaphore_wait(barrier, QUAD + has_up.astype(jnp.int32) + has_down.astype(jnp.int32))

    def block(slot, k):
        return win.at[slot * QUAD + lane + off(k), :, pl.ds(0, 2 * HD)]

    def kv_quad(k):
        return remote(kv_ref.at[lane + off(k)], win.at[top_slot * QUAD + lane, :, pl.ds(0, 2 * HD)],
                      kq_s.at[k], kq_r.at[k], me + off(k))

    def kv_quad_in(k):
        return remote(block(top_slot, k), block(top_slot, k), kq_s.at[k], kq_r.at[k], me + off(k))

    def source(slot, k):
        return kv_ref.at[lane] if slot == top_slot and k == 0 else block(slot, k)

    def z_kv(slot, k):
        return remote(source(slot, k), block(slot - 2, k),
                      zs.at[(top_slot - slot) // 2, k], zr.at[(top_slot - slot) // 2, k], up)

    def y_kv(slot, target, k):
        level = (top_slot - 1 - target) // 2
        return remote(source(slot, k), block(target, k), ys.at[level, k], yr.at[level, k], me + dy)

    def there(slot):
        return quad - top_slot + slot >= 0

    def forward_kv(slot, k, act):
        if slot >= 2:
            @pl.when(there(slot) & has_up)
            def _():
                act(z_kv(slot, k))
        if slot >= 1:
            @pl.when(there(slot) & (y == 0))
            def _():
                act(y_kv(slot, slot - 1, k))
        if slot + 1 < top_slot:
            @pl.when(there(slot) & (y == 1))
            def _():
                act(y_kv(slot, slot + 1, k))

    def q_quad(k):
        lanes = pl.ds(pl.multiple_of((lane + off(k)) * width, width), width)
        return remote(q_ref.at[:, lanes], qbuf.at[k], qs.at[k], qr.at[k], me + off(k))

    def code_up(k):
        unit = cbuf.at[quad - 2 * k] if not isinstance(k, int) or k > 0 else codes_ref
        return remote(unit, cbuf.at[quad - 2 * k], up_s.at[k + 1], up_r.at[k + 1], up)

    def code_up_in(k):
        unit = cbuf.at[quad - 2 * k]
        return remote(unit, unit, up_s.at[k], up_r.at[k], up)

    def code_down(k):
        unit = cbuf.at[quad + 2 * k] if not isinstance(k, int) or k > 0 else codes_ref
        return remote(unit, cbuf.at[quad + 2 * k], dn_s.at[k + 1], dn_r.at[k + 1], down)

    def code_down_in(k):
        unit = cbuf.at[quad + 2 * k]
        return remote(unit, unit, dn_s.at[k], dn_r.at[k], down)

    def code_y(plane):
        unit = cbuf.at[plane * 2 + y]
        return remote(unit, unit, cy_s.at[plane], cy_r.at[plane], me + dy)

    def code_y_in(plane):
        unit = cbuf.at[plane * 2 + 1 - y]
        return remote(unit, unit, cy_s.at[plane], cy_r.at[plane], me + dy)

    for k in (2, 3, 1):
        kv_quad(k).start()
    forward_kv(top_slot, 0, lambda copy: copy.start())

    @pl.when(has_down)
    def _():
        code_down(0).start()
    for k in (1, 2, 3):
        q_quad(k).start()

    window_blocks = reach + 1
    keys = window_blocks * rows
    query = lax.broadcasted_iota(jnp.int32, (rows, keys), 0)
    key = lax.broadcasted_iota(jnp.int32, (rows, keys), 1) - reach * rows
    gap = query - key
    bias[...] = jnp.where((gap >= 0) & (gap < WINDOW), 0.0, -jnp.inf).astype(F32)
    for slot in range(slots):
        value = jnp.where(there(slot), 1.0, 0.0).astype(F32)
        ones[slot * QUAD:(slot + 1) * QUAD] = jnp.full((QUAD, rows, HD), value, F32).astype(BF16)

    for k in (1, 2, 3):
        kv_quad_in(k).wait_recv()
        forward_kv(top_slot, k, lambda copy: copy.start())
    own_kv.wait()
    for slot in range(top_slot - 2, -1, -2):
        for k in range(QUAD):
            @pl.when(there(slot))
            def _():
                z_kv(slot + 2, k).wait_recv()
            forward_kv(slot, k, lambda copy: copy.start())

    own_codes.wait()

    @pl.when(has_up)
    def _():
        code_up(0).start()
    code_y(z).start()

    for slot in range(top_slot):
        @pl.when(jnp.logical_not(there(slot)))
        def _():
            first = win[top_slot * QUAD, 0:1, 0:HD].astype(F32)
            fill = jnp.concatenate([jnp.broadcast_to(first, (rows, HD)), jnp.zeros((rows, HD), F32)], axis=1)
            fill = fill.astype(BF16)
            for i in range(QUAD):
                win[slot * QUAD + i] = fill

    for slot in range(top_slot - 1, -1, -2):
        for k in range(QUAD):
            @pl.when(there(slot))
            def _():
                level = (top_slot - 1 - slot) // 2
                remote(block(slot, k), block(slot, k), ys.at[level, k], yr.at[level, k], me + dy).wait_recv()
    own_q.wait()

    def relay(k):
        @pl.when(z - k >= 0)
        def _():
            code_up_in(k).wait_recv()

            @pl.when(has_up)
            def _():
                code_up(k).start()
            code_y(z - k).start()

        @pl.when(z + k < planes)
        def _():
            code_down_in(k).wait_recv()

            @pl.when(has_down)
            def _():
                code_down(k).start()
            code_y(z + k).start()

    def piece(r, source_lane, half):
        start = source_lane * width + half * half_width
        return rot.at[r, :, pl.ds(pl.multiple_of(start, half_width), half_width)]

    def rot_x(t):
        ref = piece(lane + off(t // 2), lane, t % 2)
        return remote(ref, ref, rx_s.at[t], rx_r.at[t], me + dx)

    def rot_c(t):
        ref = piece(lane + off(t // 2), lane, t % 2)
        return remote(ref, ref, rc_s.at[t], rc_r.at[t], me + dc)

    def rot_x_in(t):
        k = t // 2
        ref = piece(lane + dx + (k % 2) * dc - (k // 2) * dx, lane + dx, t % 2)
        return remote(ref, ref, rx_s.at[t], rx_r.at[t], me + dx)

    def rot_f(t):
        k = t // 2
        ref = piece(lane + dx + (k % 2) * dc - (k // 2) * dx, lane + dx, t % 2)
        return remote(ref, ref, rf_s.at[t], rf_r.at[t], me + dc)

    def rot_c_in(t):
        k = t // 2
        ref = piece(lane + dc - (k % 2) * dc + (k // 2) * dx, lane + dc, t % 2)
        return remote(ref, ref, rc_s.at[t], rc_r.at[t], me + dc)

    def rot_f_in(t):
        k = t // 2
        ref = piece(lane + dc + dx - (k % 2) * dc - (k // 2) * dx, lane + dc + dx, t % 2)
        return remote(ref, ref, rf_s.at[t], rf_r.at[t], me + dc)

    def attend(t, carry):
        k = t // HALVES
        half = t % HALVES
        r = lane + off(k)

        @pl.when((half == 0) & (k > 0))
        def _():
            remote(qbuf.at[k], qbuf.at[k], qs.at[k], qr.at[k], me + off(k)).wait_recv()

        lanes = pl.ds(pl.multiple_of(half * half_width, half_width), half_width)
        q = qbuf[k, :, lanes]
        q = jnp.concatenate([q[:, h * HD:(h + 1) * HD] for h in range(PER_STEP)], axis=0)
        k_rows = win[pl.ds(r, window_blocks), :, 0:HD].reshape(keys, HD)
        v_rows = win[pl.ds(r, window_blocks), :, HD:2 * HD].reshape(keys, HD)
        v_rows = jnp.concatenate([v_rows, ones[pl.ds(r, window_blocks)].reshape(keys, HD)], axis=1)
        scores = lax.dot_general(q, k_rows, (((1,), (1,)), ((), ())), preferred_element_type=F32)
        scores = scores.reshape(PER_STEP, rows, keys) * (LOG2E / math.sqrt(HD)) + bias[...][None]
        top = jnp.max(scores, axis=-1, keepdims=True)
        weights = jnp.exp2(scores - top).astype(BF16)
        weighted = jnp.dot(weights.reshape(PER_STEP * rows, keys), v_rows, preferred_element_type=F32)
        weighted = weighted[:, :HD] / weighted[:, HD:]
        signs = sign_ref[lane * HALVES + half].astype(F32)
        signed = weighted.reshape(PER_STEP, rows, HD) * signs[:, None, :]
        signed = signed.reshape(PER_STEP * rows, HD)
        high = signed.astype(BF16)
        low = (signed - high.astype(F32)).astype(BF16)
        mixed = jnp.dot(high, had_ref[...], preferred_element_type=F32)
        mixed = mixed + jnp.dot(low, had_ref[...], preferred_element_type=F32)
        mixed = (mixed * (1.0 / math.sqrt(HD))).astype(BF16)
        start = lane * width + half * half_width
        for h in range(PER_STEP):
            rot[r, :, pl.ds(pl.multiple_of(start + h * HD, HD), HD)] = mixed[h * rows:(h + 1) * rows]

        @pl.when(t >= 1)
        def _():
            rot_x_in(t - 1).wait_recv()
            rot_f(t - 1).start()

        @pl.when(t == 3)
        def _():
            relay(1)

        @pl.when(t == 6)
        def _():
            relay(2)

        rot_x(t).start()
        rot_c(t).start()
        return carry

    lax.fori_loop(0, STEPS, attend, 0)
    rot_x_in(STEPS - 1).wait_recv()
    rot_f(STEPS - 1).start()

    def gathered(t, carry):
        rot_c_in(t).wait_recv()
        rot_f_in(t).wait_recv()
        return carry

    lax.fori_loop(0, STEPS, gathered, 0)

    chunk_heads = 8
    words = GROUP // 8

    def lanes_of(unit, source_lane):
        s = unit * QUAD + source_lane
        return pl.ds(pl.multiple_of(s * cols, cols), cols)

    def out_send(unit, k):
        target = out_ref.at[:, lanes_of(unit, lane)]
        return remote(stage.at[unit, lane + off(k)], target, os.at[unit, k], orr.at[unit, k], me + off(k))

    def out_recv(unit, k):
        target = out_ref.at[:, lanes_of(unit, lane + off(k))]
        return remote(target, target, os.at[unit, k], orr.at[unit, k], me + off(k))

    def out_own(unit):
        return pltpu.make_async_copy(stage.at[unit, lane], out_ref.at[:, lanes_of(unit, lane)], ol.at[unit])

    def project(unit):
        scale = scales_ref[:, lanes_of(unit, lane)]
        acc = jnp.zeros((QUAD * rows, cols), F32)
        for chunk in range(HEADS // chunk_heads):
            parts = []
            for h in range(chunk * chunk_heads, (chunk + 1) * chunk_heads):
                word = cbuf[unit, h * words:(h + 1) * words, :] ^ jnp.int32(-2004318072)
                factor = jnp.broadcast_to(scale[h:h + 1, :], (words, cols))
                for k in range(8):
                    code = jnp.right_shift(jnp.left_shift(word, 28 - 4 * k), 28)
                    parts.append(code.astype(F32).astype(BF16) * factor)
            weight = jnp.concatenate(parts, axis=0)
            span = chunk_heads * HD
            lhs = rot[:, :, chunk * span:(chunk + 1) * span].reshape(QUAD * rows, span)
            acc = acc + jnp.dot(lhs, weight, preferred_element_type=F32)
        acc = acc.astype(BF16).reshape(QUAD, rows, cols)
        stage[unit] = acc
        for k in (2, 3, 1):
            out_send(unit, k).start()
        out_own(unit).start()

    def sweep(k, carry):
        @pl.when(k >= 3)
        def _():
            relay(k)

        def one(j, inner):
            side, other = j // 2, j % 2
            plane = z + k * (2 * side - 1)

            @pl.when((plane >= 0) & (plane < planes) & ((k > 0) | (side == 0)))
            def _():
                @pl.when(other == 1)
                def _():
                    code_y_in(plane).wait_recv()
                project(plane * 2 + y + other * (1 - 2 * y))

            return inner

        lax.fori_loop(0, 4, one, 0)
        return carry

    lax.fori_loop(0, planes, sweep, 0)

    for k in (1, 2, 3):
        kv_quad(k).wait_send()
        q_quad(k).wait_send()
    for slot in range(top_slot, -1, -2):
        for k in range(QUAD):
            forward_kv(slot, k, lambda copy: copy.wait_send())

    def drain_codes(k, carry):
        @pl.when((z - k >= 0) & has_up)
        def _():
            code_up(k).wait_send()

        @pl.when((z + k < planes) & has_down)
        def _():
            code_down(k).wait_send()
        code_y(k).wait_send()
        return carry

    lax.fori_loop(0, planes, drain_codes, 0)

    def drain_rot(t, carry):
        rot_x(t).wait_send()
        rot_c(t).wait_send()
        rot_f(t).wait_send()
        return carry

    lax.fori_loop(0, STEPS, drain_rot, 0)

    def drain_out(unit, carry):
        out_own(unit).wait()
        for k in (1, 2, 3):
            out_send(unit, k).wait_send()
            out_recv(unit, k).wait_recv()
        return carry

    lax.fori_loop(0, 2 * planes, drain_out, 0)


def on_device(queries, keys_values, head_signs, out_codes, out_scales):
    n = lax.axis_size("seq")
    rows = queries.shape[0]
    reach = (WINDOW + rows - 2) // rows
    span = -(-reach // QUAD)
    slots = span + 1
    assert slots % 2 == 1
    planes = n // (2 * QUAD)
    word_rows, cols = out_codes.shape
    vmem = pl.BlockSpec(memory_space=pltpu.VMEM)
    dma = pltpu.SemaphoreType.DMA
    per_head = keys_values.reshape(rows, 2, KV, HD).transpose(2, 0, 1, 3).reshape(KV, rows, 2 * HD)
    return pl.pallas_call(
        functools.partial(kernel, n, reach, slots),
        out_shape=jax.ShapeDtypeStruct((rows, n * cols), BF16),
        in_specs=[vmem] * 6,
        out_specs=pl.BlockSpec(memory_space=pl.ANY),
        scratch_shapes=[
            pltpu.VMEM((slots * QUAD, rows, 2 * HD), BF16),
            pltpu.VMEM((slots * QUAD, rows, HD), BF16),
            pltpu.VMEM((QUAD, rows, LANE_HEADS * HD), BF16),
            pltpu.VMEM((2 * planes, word_rows, cols), jnp.int32),
            pltpu.VMEM((QUAD, rows, HEADS * HD), BF16),
            pltpu.VMEM((rows, (reach + 1) * rows), F32),
            pltpu.VMEM((2 * planes, QUAD, rows, cols), BF16),
            dma((3,)),
            dma((QUAD,)), dma((QUAD,)),
            dma((QUAD,)), dma((QUAD,)),
            dma((slots // 2, QUAD)), dma((slots // 2, QUAD)),
            dma((slots // 2, QUAD)), dma((slots // 2, QUAD)),
            dma((planes + 1,)), dma((planes + 1,)),
            dma((planes + 1,)), dma((planes + 1,)),
            dma((planes,)), dma((planes,)),
            dma((STEPS,)), dma((STEPS,)),
            dma((STEPS,)), dma((STEPS,)),
            dma((STEPS,)), dma((STEPS,)),
            dma((2 * planes, QUAD)), dma((2 * planes, QUAD)),
            dma((2 * planes,)),
        ],
        compiler_params=pltpu.CompilerParams(
            collective_id=0, has_side_effects=True, vmem_limit_bytes=64 * 1000 * 1000
        ),
    )(
        queries,
        per_head,
        head_signs.reshape(STEPS, PER_STEP, HD),
        reordered_hadamard(),
        out_codes,
        out_scales,
    )


def solution(mesh):
    return jax.shard_map(
        on_device,
        mesh=mesh,
        in_specs=(
            P(("groups", "seq"), None),
            P(("groups", "seq"), None, None),
            P(),
            P(None, "seq"),
            P(),
        ),
        out_specs=P(("groups", "seq"), None),
        check_vma=False,
    )
```

```python
import functools
import math

import jax
import jax.numpy as jnp
from jax import lax
from jax.experimental import pallas as pl
from jax.experimental.pallas import tpu as pltpu
from jax.sharding import PartitionSpec as P

HEADS = 32
KV = 4
HD = 128
GROUP = 128
WINDOW = 2048
QUAD = 4
LANE_HEADS = HEADS // QUAD
HALVES = 2
PER_STEP = LANE_HEADS // HALVES
STEPS = QUAD * HALVES
LAG = 3
LOG2E = 1.4426950408889634
MESH = pl.DeviceIdType.MESH
BF16 = jnp.bfloat16
F32 = jnp.float32


def reordered_hadamard():
    column = jnp.arange(HD, dtype=jnp.int32)
    source = (column % 16) * 8 + column // 16
    common = jnp.bitwise_and(jnp.arange(HD, dtype=jnp.int32)[:, None], source[None, :])
    ones = jnp.zeros((HD, HD), jnp.int32)
    for bit in range(HD.bit_length()):
        ones = ones + jnp.bitwise_and(jnp.right_shift(common, bit), 1)
    return jnp.where(ones % 2 == 0, 1.0, -1.0).astype(BF16)


def kernel(
    n, reach, slots,
    q_ref, kv_ref, sign_ref, had_ref, codes_ref, scales_ref, out_ref,
    win, ones, qbuf, cbuf, rot, bias, stage, local_sem,
    kq_s, kq_r, qs, qr, zs, zr, ys, yr, up_s, up_r, dn_s, dn_r, cy_s, cy_r,
    rx_s, rx_r, rc_s, rc_r, rf_s, rf_r, os, orr, ol,
):
    rows = q_ref.shape[0]
    cols = codes_ref.shape[1]
    planes = n // (2 * QUAD)
    width = LANE_HEADS * HD
    half_width = PER_STEP * HD
    top_slot = slots - 1
    me = lax.axis_index("seq")
    z = me // (2 * QUAD)
    y = (me // QUAD) % 2
    lane = me % QUAD
    quad = me // QUAD
    core, x = lane % 2, lane // 2
    dc, dx, dy = 1 - 2 * core, 2 - 4 * x, QUAD - 2 * QUAD * y
    up, down = me + 2 * QUAD, me - 2 * QUAD
    has_up, has_down = z + 1 < planes, z >= 1

    def off(k):
        return (k % 2) * dc + (k // 2) * dx

    def remote(src, dst, send, recv, target):
        return pltpu.make_async_remote_copy(
            src_ref=src, dst_ref=dst, send_sem=send, recv_sem=recv,
            device_id={"seq": target}, device_id_type=MESH,
        )

    barrier = pltpu.get_barrier_semaphore()

    def greet(target):
        pl.semaphore_signal(barrier, inc=1, device_id={"seq": target}, device_id_type=MESH)

    for k in (2, 3, 1):
        greet(me + off(k))
    greet(me + dy)

    @pl.when(has_up)
    def _():
        greet(up)

    @pl.when(has_down)
    def _():
        greet(down)

    own_kv = pltpu.make_async_copy(
        kv_ref.at[lane], win.at[top_slot * QUAD + lane, :, pl.ds(0, 2 * HD)], local_sem.at[0])
    own_lanes = pl.ds(pl.multiple_of(lane * width, width), width)
    own_q = pltpu.make_async_copy(q_ref.at[:, own_lanes], qbuf.at[0], local_sem.at[1])
    own_codes = pltpu.make_async_copy(codes_ref, cbuf.at[quad], local_sem.at[2])
    own_kv.start()
    own_q.start()
    own_codes.start()

    pl.semaphore_wait(barrier, QUAD + has_up.astype(jnp.int32) + has_down.astype(jnp.int32))

    def block(slot, k):
        return win.at[slot * QUAD + lane + off(k), :, pl.ds(0, 2 * HD)]

    def kv_quad(k):
        return remote(kv_ref.at[lane + off(k)], win.at[top_slot * QUAD + lane, :, pl.ds(0, 2 * HD)],
                      kq_s.at[k], kq_r.at[k], me + off(k))

    def kv_quad_in(k):
        return remote(block(top_slot, k), block(top_slot, k), kq_s.at[k], kq_r.at[k], me + off(k))

    def source(slot, k):
        return kv_ref.at[lane] if slot == top_slot and k == 0 else block(slot, k)

    def z_kv(slot, k):
        return remote(source(slot, k), block(slot - 2, k),
                      zs.at[(top_slot - slot) // 2, k], zr.at[(top_slot - slot) // 2, k], up)

    def y_kv(slot, target, k):
        level = (top_slot - 1 - target) // 2
        return remote(source(slot, k), block(target, k), ys.at[level, k], yr.at[level, k], me + dy)

    def there(slot):
        return quad - top_slot + slot >= 0

    def forward_kv(slot, k, act):
        if slot >= 2:
            @pl.when(there(slot) & has_up)
            def _():
                act(z_kv(slot, k))
        if slot >= 1:
            @pl.when(there(slot) & (y == 0))
            def _():
                act(y_kv(slot, slot - 1, k))
        if slot + 1 < top_slot:
            @pl.when(there(slot) & (y == 1))
            def _():
                act(y_kv(slot, slot + 1, k))

    def q_quad(k):
        lanes = pl.ds(pl.multiple_of((lane + off(k)) * width, width), width)
        return remote(q_ref.at[:, lanes], qbuf.at[k], qs.at[k], qr.at[k], me + off(k))

    def code_up(k):
        unit = cbuf.at[quad - 2 * k] if not isinstance(k, int) or k > 0 else codes_ref
        return remote(unit, cbuf.at[quad - 2 * k], up_s.at[k + 1], up_r.at[k + 1], up)

    def code_up_in(k):
        unit = cbuf.at[quad - 2 * k]
        return remote(unit, unit, up_s.at[k], up_r.at[k], up)

    def code_down(k):
        unit = cbuf.at[quad + 2 * k] if not isinstance(k, int) or k > 0 else codes_ref
        return remote(unit, cbuf.at[quad + 2 * k], dn_s.at[k + 1], dn_r.at[k + 1], down)

    def code_down_in(k):
        unit = cbuf.at[quad + 2 * k]
        return remote(unit, unit, dn_s.at[k], dn_r.at[k], down)

    def code_y(plane):
        unit = cbuf.at[plane * 2 + y]
        return remote(unit, unit, cy_s.at[plane], cy_r.at[plane], me + dy)

    def code_y_in(plane):
        unit = cbuf.at[plane * 2 + 1 - y]
        return remote(unit, unit, cy_s.at[plane], cy_r.at[plane], me + dy)

    near = jnp.minimum(z, planes - 1 - z)
    toward = jnp.where(z <= planes - 1 - z, 1, -1)

    def plane_at(p):
        both = z + ((p + 1) // 2) * (2 * (p % 2) - 1)
        return jnp.where(p <= 2 * near, both, z + toward * (p - near))

    begin = jnp.where(z == 0, 125, jnp.where(z == 1, 186, jnp.where(z == 2, 220, 200)))
    due = [None]
    for p in range(1, planes):
        d = plane_at(p) - z
        arrival = jnp.where(d > 0, 53 + 130 * d, jnp.where(z == 1, 123, 183) - 117 * d)
        step = jnp.maximum((arrival - begin - 17) // 33, 0)
        step = jnp.where((d == 1) & has_down, -1, step)
        due.append(step if p == 1 else jnp.maximum(due[-1], step))

    def relay(p):
        plane = plane_at(p)

        @pl.when(plane < z)
        def _():
            code_up_in(z - plane).wait_recv()

            @pl.when(has_up)
            def _():
                code_up(z - plane).start()
            code_y(plane).start()

        @pl.when(plane > z)
        def _():
            code_down_in(plane - z).wait_recv()

            @pl.when(has_down)
            def _():
                code_down(plane - z).start()
            code_y(plane).start()

    for k in (2, 3, 1):
        kv_quad(k).start()
    forward_kv(top_slot, 0, lambda copy: copy.start())

    @pl.when(has_down)
    def _():
        code_down(0).start()
    for k in (1, 2, 3):
        q_quad(k).start()

    window_blocks = reach + 1
    keys = window_blocks * rows
    query = lax.broadcasted_iota(jnp.int32, (rows, keys), 0)
    key = lax.broadcasted_iota(jnp.int32, (rows, keys), 1) - reach * rows
    gap = query - key
    bias[...] = jnp.where((gap >= 0) & (gap < WINDOW), 0.0, -jnp.inf).astype(F32)
    for slot in range(slots):
        value = jnp.where(there(slot), 1.0, 0.0).astype(F32)
        ones[slot * QUAD:(slot + 1) * QUAD] = jnp.full((QUAD, rows, HD), value, F32).astype(BF16)

    for k in (1, 2, 3):
        kv_quad_in(k).wait_recv()
        forward_kv(top_slot, k, lambda copy: copy.start())
    own_kv.wait()
    for slot in range(top_slot - 2, -1, -2):
        for k in range(QUAD):
            @pl.when(there(slot))
            def _():
                z_kv(slot + 2, k).wait_recv()
            forward_kv(slot, k, lambda copy: copy.start())
        if slot in (top_slot - 2, 0):
            if slot == top_slot - 2:
                own_codes.wait()

                @pl.when(has_up)
                def _():
                    code_up(0).start()

            @pl.when(y == (0 if slot == top_slot - 2 else 1))
            def _():
                code_y(z).start()

    for p in range(1, planes):
        @pl.when(due[p] < 0)
        def _():
            relay(p)

    for slot in range(top_slot):
        @pl.when(jnp.logical_not(there(slot)))
        def _():
            first = win[top_slot * QUAD, 0:1, 0:HD].astype(F32)
            fill = jnp.concatenate([jnp.broadcast_to(first, (rows, HD)), jnp.zeros((rows, HD), F32)], axis=1)
            fill = fill.astype(BF16)
            for i in range(QUAD):
                win[slot * QUAD + i] = fill

    for slot in range(top_slot - 1, -1, -2):
        for k in range(QUAD):
            @pl.when(there(slot))
            def _():
                level = (top_slot - 1 - slot) // 2
                remote(block(slot, k), block(slot, k), ys.at[level, k], yr.at[level, k], me + dy).wait_recv()
    own_q.wait()

    def piece(r, source_lane, half):
        start = source_lane * width + half * half_width
        return rot.at[r, :, pl.ds(pl.multiple_of(start, half_width), half_width)]

    def rot_x(t):
        ref = piece(lane + off(t // 2), lane, t % 2)
        return remote(ref, ref, rx_s.at[t], rx_r.at[t], me + dx)

    def rot_c(t):
        ref = piece(lane + off(t // 2), lane, t % 2)
        return remote(ref, ref, rc_s.at[t], rc_r.at[t], me + dc)

    def rot_x_in(t):
        k = t // 2
        ref = piece(lane + dx + (k % 2) * dc - (k // 2) * dx, lane + dx, t % 2)
        return remote(ref, ref, rx_s.at[t], rx_r.at[t], me + dx)

    def rot_f(t):
        k = t // 2
        ref = piece(lane + dx + (k % 2) * dc - (k // 2) * dx, lane + dx, t % 2)
        return remote(ref, ref, rf_s.at[t], rf_r.at[t], me + dc)

    def rot_c_in(t):
        k = t // 2
        ref = piece(lane + dc - (k % 2) * dc + (k // 2) * dx, lane + dc, t % 2)
        return remote(ref, ref, rc_s.at[t], rc_r.at[t], me + dc)

    def rot_f_in(t):
        k = t // 2
        ref = piece(lane + dc + dx - (k % 2) * dc - (k // 2) * dx, lane + dc + dx, t % 2)
        return remote(ref, ref, rf_s.at[t], rf_r.at[t], me + dc)

    def attend(t, carry):
        k = t // HALVES
        half = t % HALVES
        r = lane + off(k)

        @pl.when((half == 0) & (k > 0))
        def _():
            remote(qbuf.at[k], qbuf.at[k], qs.at[k], qr.at[k], me + off(k)).wait_recv()

        lanes = pl.ds(pl.multiple_of(half * half_width, half_width), half_width)
        q = qbuf[k, :, lanes]
        q = jnp.concatenate([q[:, h * HD:(h + 1) * HD] for h in range(PER_STEP)], axis=0)
        k_rows = win[pl.ds(r, window_blocks), :, 0:HD].reshape(keys, HD)
        v_rows = win[pl.ds(r, window_blocks), :, HD:2 * HD].reshape(keys, HD)
        v_rows = jnp.concatenate([v_rows, ones[pl.ds(r, window_blocks)].reshape(keys, HD)], axis=1)
        scores = lax.dot_general(q, k_rows, (((1,), (1,)), ((), ())), preferred_element_type=F32)
        scores = scores.reshape(PER_STEP, rows, keys) * (LOG2E / math.sqrt(HD)) + bias[...][None]
        top = jnp.max(scores, axis=-1, keepdims=True)
        weights = jnp.exp2(scores - top).astype(BF16)
        weighted = jnp.dot(weights.reshape(PER_STEP * rows, keys), v_rows, preferred_element_type=F32)
        weighted = weighted[:, :HD] / weighted[:, HD:]
        signs = sign_ref[lane * HALVES + half].astype(F32)
        signed = weighted.reshape(PER_STEP, rows, HD) * signs[:, None, :]
        signed = signed.reshape(PER_STEP * rows, HD)
        high = signed.astype(BF16)
        low = (signed - high.astype(F32)).astype(BF16)
        mixed = jnp.dot(high, had_ref[...], preferred_element_type=F32)
        mixed = mixed + jnp.dot(low, had_ref[...], preferred_element_type=F32)
        mixed = (mixed * (1.0 / math.sqrt(HD))).astype(BF16)
        start = lane * width + half * half_width
        for h in range(PER_STEP):
            rot[r, :, pl.ds(pl.multiple_of(start + h * HD, HD), HD)] = mixed[h * rows:(h + 1) * rows]

        @pl.when(t >= LAG)
        def _():
            rot_x_in(t - LAG).wait_recv()
            rot_f(t - LAG).start()

        for p in range(1, planes):
            @pl.when(t == due[p])
            def _():
                relay(p)

        rot_x(t).start()
        rot_c(t).start()
        return carry

    lax.fori_loop(0, STEPS, attend, 0)
    def gathered(t, carry):
        rot_c_in(t).wait_recv()
        return carry

    def gathered_far(t, carry):
        rot_f_in(t).wait_recv()
        return carry

    lax.fori_loop(0, STEPS, gathered, 0)
    lax.fori_loop(0, STEPS // 2, gathered_far, 0)
    chunk_heads = 8
    words = GROUP // 8

    def lanes_of(unit, source_lane):
        s = unit * QUAD + source_lane
        return pl.ds(pl.multiple_of(s * cols, cols), cols)

    def out_send(unit, k):
        target = out_ref.at[:, lanes_of(unit, lane)]
        return remote(stage.at[unit, lane + off(k)], target, os.at[unit, k], orr.at[unit, k], me + off(k))

    def out_recv(unit, k):
        target = out_ref.at[:, lanes_of(unit, lane + off(k))]
        return remote(target, target, os.at[unit, k], orr.at[unit, k], me + off(k))

    def out_own(unit):
        return pltpu.make_async_copy(stage.at[unit, lane], out_ref.at[:, lanes_of(unit, lane)], ol.at[unit])

    def project(unit, side):
        scale = scales_ref[:, lanes_of(unit, lane)]
        acc = jnp.zeros((2 * rows, cols), F32)
        for chunk in range(HEADS // chunk_heads):
            parts = []
            for h in range(chunk * chunk_heads, (chunk + 1) * chunk_heads):
                word = cbuf[unit, h * words:(h + 1) * words, :] ^ jnp.int32(-2004318072)
                factor = jnp.broadcast_to(scale[h:h + 1, :], (words, cols))
                for k in range(8):
                    code = jnp.right_shift(jnp.left_shift(word, 28 - 4 * k), 28)
                    parts.append(code.astype(F32).astype(BF16) * factor)
            weight = jnp.concatenate(parts, axis=0)
            span = chunk_heads * HD
            lhs = rot[pl.ds(2 * side, 2), :, chunk * span:(chunk + 1) * span].reshape(2 * rows, span)
            acc = acc + jnp.dot(lhs, weight, preferred_element_type=F32)
        stage[unit, pl.ds(2 * side, 2)] = acc.astype(BF16).reshape(2, rows, cols)

        @pl.when(side == x)
        def _():
            out_send(unit, 1).start()
            out_own(unit).start()

        @pl.when(side != x)
        def _():
            out_send(unit, 2).start()
            out_send(unit, 3).start()

    def sweep(i, carry):
        early = i < 2 * planes
        j = i % planes
        q = jnp.where(early, j, planes + (i - 2 * planes) // 2)
        partner = jnp.where(early, i < planes, i % 2 == 0)
        plane = plane_at(q // 2)
        other = q % 2

        @pl.when(i == jnp.where(z == 0, planes, 2 * planes))
        def _():
            for p in range(1, planes):
                @pl.when(due[p] >= STEPS)
                def _():
                    relay(p)

        @pl.when(partner & (other == 1))
        def _():
            code_y_in(plane).wait_recv()

        @pl.when(i == planes)
        def _():
            for t in range(STEPS - LAG, STEPS):
                rot_x_in(t).wait_recv()
                rot_f(t).start()
            lax.fori_loop(STEPS // 2, STEPS, gathered_far, 0)
        project(plane * 2 + y + other * (1 - 2 * y), jnp.where(partner, 1 - x, x))
        return carry

    lax.fori_loop(0, 4 * planes, sweep, 0)

    for k in (1, 2, 3):
        kv_quad(k).wait_send()
        q_quad(k).wait_send()
    for slot in range(top_slot, -1, -2):
        for k in range(QUAD):
            forward_kv(slot, k, lambda copy: copy.wait_send())

    def drain_codes(k, carry):
        @pl.when((z - k >= 0) & has_up)
        def _():
            code_up(k).wait_send()

        @pl.when((z + k < planes) & has_down)
        def _():
            code_down(k).wait_send()
        code_y(k).wait_send()
        return carry

    lax.fori_loop(0, planes, drain_codes, 0)

    def drain_rot(t, carry):
        rot_x(t).wait_send()
        rot_c(t).wait_send()
        rot_f(t).wait_send()
        return carry

    lax.fori_loop(0, STEPS, drain_rot, 0)

    def drain_out(unit, carry):
        out_own(unit).wait()
        for k in (1, 2, 3):
            out_send(unit, k).wait_send()
            out_recv(unit, k).wait_recv()
        return carry

    lax.fori_loop(0, 2 * planes, drain_out, 0)


def on_device(queries, keys_values, head_signs, out_codes, out_scales):
    n = lax.axis_size("seq")
    rows = queries.shape[0]
    reach = (WINDOW + rows - 2) // rows
    span = -(-reach // QUAD)
    slots = span + 1
    assert slots % 2 == 1
    planes = n // (2 * QUAD)
    word_rows, cols = out_codes.shape
    vmem = pl.BlockSpec(memory_space=pltpu.VMEM)
    dma = pltpu.SemaphoreType.DMA
    per_head = keys_values.reshape(rows, 2, KV, HD).transpose(2, 0, 1, 3).reshape(KV, rows, 2 * HD)
    return pl.pallas_call(
        functools.partial(kernel, n, reach, slots),
        out_shape=jax.ShapeDtypeStruct((rows, n * cols), BF16),
        in_specs=[vmem] * 6,
        out_specs=pl.BlockSpec(memory_space=pl.ANY),
        scratch_shapes=[
            pltpu.VMEM((slots * QUAD, rows, 2 * HD), BF16),
            pltpu.VMEM((slots * QUAD, rows, HD), BF16),
            pltpu.VMEM((QUAD, rows, LANE_HEADS * HD), BF16),
            pltpu.VMEM((2 * planes, word_rows, cols), jnp.int32),
            pltpu.VMEM((QUAD, rows, HEADS * HD), BF16),
            pltpu.VMEM((rows, (reach + 1) * rows), F32),
            pltpu.VMEM((2 * planes, QUAD, rows, cols), BF16),
            dma((3,)),
            dma((QUAD,)), dma((QUAD,)),
            dma((QUAD,)), dma((QUAD,)),
            dma((slots // 2, QUAD)), dma((slots // 2, QUAD)),
            dma((slots // 2, QUAD)), dma((slots // 2, QUAD)),
            dma((planes + 1,)), dma((planes + 1,)),
            dma((planes + 1,)), dma((planes + 1,)),
            dma((planes,)), dma((planes,)),
            dma((STEPS,)), dma((STEPS,)),
            dma((STEPS,)), dma((STEPS,)),
            dma((STEPS,)), dma((STEPS,)),
            dma((2 * planes, QUAD)), dma((2 * planes, QUAD)),
            dma((2 * planes,)),
        ],
        compiler_params=pltpu.CompilerParams(
            collective_id=0, has_side_effects=True, vmem_limit_bytes=64 * 1000 * 1000
        ),
    )(
        queries,
        per_head,
        head_signs.reshape(STEPS, PER_STEP, HD),
        reordered_hadamard(),
        out_codes,
        out_scales,
    )


def solution(mesh):
    return jax.shard_map(
        on_device,
        mesh=mesh,
        in_specs=(
            P(("groups", "seq"), None),
            P(("groups", "seq"), None, None),
            P(),
            P(None, "seq"),
            P(),
        ),
        out_specs=P(("groups", "seq"), None),
        check_vma=False,
    )
```

```python
import functools
import math

import jax
import jax.numpy as jnp
from jax import lax
from jax.experimental import pallas as pl
from jax.experimental.pallas import tpu as pltpu
from jax.sharding import PartitionSpec as P

HEADS = 32
KV = 4
HD = 128
GROUP = 128
WINDOW = 2048
QUAD = 4
LANE_HEADS = HEADS // QUAD
HALVES = 2
PER_STEP = LANE_HEADS // HALVES
STEPS = QUAD * HALVES
LAG = 3
LOG2E = 1.4426950408889634
MESH = pl.DeviceIdType.MESH
BF16 = jnp.bfloat16
F32 = jnp.float32


def reordered_hadamard():
    column = jnp.arange(HD, dtype=jnp.int32)
    source = (column % 16) * 8 + column // 16
    common = jnp.bitwise_and(jnp.arange(HD, dtype=jnp.int32)[:, None], source[None, :])
    ones = jnp.zeros((HD, HD), jnp.int32)
    for bit in range(HD.bit_length()):
        ones = ones + jnp.bitwise_and(jnp.right_shift(common, bit), 1)
    return jnp.where(ones % 2 == 0, 1.0, -1.0).astype(BF16)


def kernel(
    n, reach, slots,
    q_ref, kv_ref, sign_ref, had_ref, codes_ref, scales_ref, out_ref,
    win, ones, qbuf, cbuf, rot, bias, sbuf, wbuf, stage,
    q_all, signs_buf, scales, local_sem,
    kq_s, kq_r, qs, qr, zs, zr, ys, yr, up_s, up_r, dn_s, dn_r, cy_s, cy_r,
    rx_s, rx_r, rc_s, rc_r, rf_s, rf_r, os, orr, ol,
):
    rows = q_ref.shape[0]
    cols = codes_ref.shape[1]
    planes = n // (2 * QUAD)
    width = LANE_HEADS * HD
    half_width = PER_STEP * HD
    top_slot = slots - 1
    me = lax.axis_index("seq")
    z = me // (2 * QUAD)
    y = (me // QUAD) % 2
    lane = me % QUAD
    quad = me // QUAD
    core, x = lane % 2, lane // 2
    dc, dx, dy = 1 - 2 * core, 2 - 4 * x, QUAD - 2 * QUAD * y
    up, down = me + 2 * QUAD, me - 2 * QUAD
    has_up, has_down = z + 1 < planes, z >= 1

    def off(k):
        return (k % 2) * dc + (k // 2) * dx

    def remote(src, dst, send, recv, target):
        return pltpu.make_async_remote_copy(
            src_ref=src, dst_ref=dst, send_sem=send, recv_sem=recv,
            device_id={"seq": target}, device_id_type=MESH,
        )

    own_kv = pltpu.make_async_copy(
        kv_ref.at[lane], win.at[top_slot * QUAD + lane, :, pl.ds(0, 2 * HD)], local_sem.at[0])
    own_lanes = pl.ds(pl.multiple_of(lane * width, width), width)
    all_q = pltpu.make_async_copy(q_ref, q_all, local_sem.at[5])
    own_q = pltpu.make_async_copy(q_ref.at[:, own_lanes], qbuf.at[0], local_sem.at[1])
    own_codes = pltpu.make_async_copy(codes_ref, cbuf.at[quad], local_sem.at[2])
    all_signs = pltpu.make_async_copy(sign_ref, signs_buf, local_sem.at[3])
    all_scales = pltpu.make_async_copy(scales_ref, scales, local_sem.at[4])
    for copy in (own_kv, all_q, own_codes, own_q, all_signs, all_scales):
        copy.start()

    barrier = pltpu.get_barrier_semaphore()

    def greet(target):
        pl.semaphore_signal(barrier, inc=1, device_id={"seq": target}, device_id_type=MESH)

    for k in (2, 3, 1):
        greet(me + off(k))
    greet(me + dy)

    @pl.when(has_up)
    def _():
        greet(up)

    @pl.when(has_down)
    def _():
        greet(down)

    pl.semaphore_wait(barrier, QUAD + has_up.astype(jnp.int32) + has_down.astype(jnp.int32))

    def block(slot, k):
        return win.at[slot * QUAD + lane + off(k), :, pl.ds(0, 2 * HD)]

    def kv_quad(k):
        return remote(kv_ref.at[lane + off(k)], win.at[top_slot * QUAD + lane, :, pl.ds(0, 2 * HD)],
                      kq_s.at[k], kq_r.at[k], me + off(k))

    def kv_quad_in(k):
        return remote(block(top_slot, k), block(top_slot, k), kq_s.at[k], kq_r.at[k], me + off(k))

    def source(slot, k):
        return kv_ref.at[lane] if slot == top_slot and k == 0 else block(slot, k)

    def z_kv(slot, k):
        return remote(source(slot, k), block(slot - 2, k),
                      zs.at[(top_slot - slot) // 2, k], zr.at[(top_slot - slot) // 2, k], up)

    def y_kv(slot, target, k):
        level = (top_slot - 1 - target) // 2
        return remote(source(slot, k), block(target, k), ys.at[level, k], yr.at[level, k], me + dy)

    def there(slot):
        return quad - top_slot + slot >= 0

    def forward_kv(slot, k, act):
        if slot >= 2:
            @pl.when(there(slot) & has_up)
            def _():
                act(z_kv(slot, k))
        if slot >= 1:
            @pl.when(there(slot) & (y == 0))
            def _():
                act(y_kv(slot, slot - 1, k))
        if slot + 1 < top_slot:
            @pl.when(there(slot) & (y == 1))
            def _():
                act(y_kv(slot, slot + 1, k))

    def q_quad(k):
        lanes = pl.ds(pl.multiple_of((lane + off(k)) * width, width), width)
        return remote(q_all.at[:, lanes], qbuf.at[k], qs.at[k], qr.at[k], me + off(k))

    def code_up(k):
        unit = cbuf.at[quad - 2 * k]
        return remote(unit, unit, up_s.at[k + 1], up_r.at[k + 1], up)

    def code_up_in(k):
        unit = cbuf.at[quad - 2 * k]
        return remote(unit, unit, up_s.at[k], up_r.at[k], up)

    def code_down(k):
        unit = cbuf.at[quad + 2 * k]
        return remote(unit, unit, dn_s.at[k + 1], dn_r.at[k + 1], down)

    def code_down_in(k):
        unit = cbuf.at[quad + 2 * k]
        return remote(unit, unit, dn_s.at[k], dn_r.at[k], down)

    def code_y(plane):
        unit = cbuf.at[plane * 2 + y]
        return remote(unit, unit, cy_s.at[plane], cy_r.at[plane], me + dy)

    def code_y_in(plane):
        unit = cbuf.at[plane * 2 + 1 - y]
        return remote(unit, unit, cy_s.at[plane], cy_r.at[plane], me + dy)

    near = jnp.minimum(z, planes - 1 - z)
    toward = jnp.where(z <= planes - 1 - z, 1, -1)

    def plane_at(p):
        both = z + ((p + 1) // 2) * (2 * (p % 2) - 1)
        return jnp.where(p <= 2 * near, both, z + toward * (p - near))

    begin = jnp.where(z == 0, 80, jnp.where(z == 1, 138, 175))
    due, item_due = [None], [None]
    early = planes + 1
    for p in range(1, planes):
        d = plane_at(p) - z
        arrival = jnp.where(d > 0, 130 * d, jnp.where(z == 1, 71, 130) - 117 * d)
        step_due = jnp.maximum((arrival - begin - 10) // 20, 0)
        step_due = jnp.where((d == 1) & has_down, -1, step_due)
        due.append(step_due if p == 1 else jnp.maximum(due[-1], step_due))
        first_use = 2 * p - 1 if 2 * p - 1 < early else 2 * early + 2 * (2 * p - 1 - early)
        item = jnp.minimum(jnp.maximum(arrival - begin - 19 * STEPS - 10, 0) // 9, first_use)
        item_due.append(item if p == 1 else jnp.maximum(item_due[-1], item))

    def relay(p):
        plane = plane_at(p)

        @pl.when(plane < z)
        def _():
            code_up_in(z - plane).wait_recv()

            @pl.when(has_up)
            def _():
                code_up(z - plane).start()
            code_y(plane).start()

        @pl.when(plane > z)
        def _():
            code_down_in(plane - z).wait_recv()

            @pl.when(has_down)
            def _():
                code_down(plane - z).start()
            code_y(plane).start()

    for k in (2, 3, 1):
        kv_quad(k).start()
    forward_kv(top_slot, 0, lambda copy: copy.start())

    own_codes.wait()

    @pl.when(has_down)
    def _():
        code_down(0).start()
    all_q.wait()
    for k in (1, 2, 3):
        q_quad(k).start()

    window_blocks = reach + 1
    keys = window_blocks * rows
    for edge, offset in ((0, reach * rows), (1, 0)):
        query = lax.broadcasted_iota(jnp.int32, (rows, rows), 0)
        key = lax.broadcasted_iota(jnp.int32, (rows, rows), 1) - offset
        gap = query - key
        bias[:, edge * rows:(edge + 1) * rows] = jnp.where((gap >= 0) & (gap < WINDOW), 0.0, -jnp.inf).astype(F32)
    for slot in range(slots):
        value = jnp.where(there(slot), 1.0, 0.0).astype(F32)
        ones[slot * QUAD:(slot + 1) * QUAD] = jnp.full((QUAD, rows, HD), value, F32).astype(BF16)

    for k in (1, 2, 3):
        kv_quad_in(k).wait_recv()
        forward_kv(top_slot, k, lambda copy: copy.start())
    own_kv.wait()
    for slot in range(top_slot - 2, -1, -2):
        for k in range(QUAD):
            @pl.when(there(slot))
            def _():
                z_kv(slot + 2, k).wait_recv()
            forward_kv(slot, k, lambda copy: copy.start())
        if slot in (top_slot - 2, 0):
            if slot == top_slot - 2:
                @pl.when(has_up)
                def _():
                    code_up(0).start()

            @pl.when(y == (0 if slot == top_slot - 2 else 1))
            def _():
                code_y(z).start()

    for p in range(1, planes):
        @pl.when(due[p] < 0)
        def _():
            relay(p)

    for slot in range(top_slot):
        @pl.when(jnp.logical_not(there(slot)))
        def _():
            first = win[top_slot * QUAD, 0:1, 0:HD].astype(F32)
            fill = jnp.concatenate([jnp.broadcast_to(first, (rows, HD)), jnp.zeros((rows, HD), F32)], axis=1)
            fill = fill.astype(BF16)
            for i in range(QUAD):
                win[slot * QUAD + i] = fill

    for slot in range(top_slot - 1, -1, -2):
        for k in range(QUAD):
            @pl.when(there(slot))
            def _():
                level = (top_slot - 1 - slot) // 2
                remote(block(slot, k), block(slot, k), ys.at[level, k], yr.at[level, k], me + dy).wait_recv()
    own_q.wait()
    all_signs.wait()
    all_scales.wait()

    def piece(r, source_lane, half):
        start = source_lane * width + half * half_width
        return rot.at[r, :, pl.ds(pl.multiple_of(start, half_width), half_width)]

    def rot_x(t):
        ref = piece(lane + off(t // 2), lane, t % 2)
        return remote(ref, ref, rx_s.at[t], rx_r.at[t], me + dx)

    def rot_c(t):
        ref = piece(lane + off(t // 2), lane, t % 2)
        return remote(ref, ref, rc_s.at[t], rc_r.at[t], me + dc)

    def rot_x_in(t):
        k = t // 2
        ref = piece(lane + dx + (k % 2) * dc - (k // 2) * dx, lane + dx, t % 2)
        return remote(ref, ref, rx_s.at[t], rx_r.at[t], me + dx)

    def rot_f(t):
        k = t // 2
        ref = piece(lane + dx + (k % 2) * dc - (k // 2) * dx, lane + dx, t % 2)
        return remote(ref, ref, rf_s.at[t], rf_r.at[t], me + dc)

    def rot_c_in(t):
        k = t // 2
        ref = piece(lane + dc - (k % 2) * dc + (k // 2) * dx, lane + dc, t % 2)
        return remote(ref, ref, rc_s.at[t], rc_r.at[t], me + dc)

    def rot_f_in(t):
        k = t // 2
        ref = piece(lane + dc + dx - (k % 2) * dc - (k // 2) * dx, lane + dc + dx, t % 2)
        return remote(ref, ref, rf_s.at[t], rf_r.at[t], me + dc)

    first_edge, last_edge = rows, keys - rows

    def score(t, slot):
        k = t // HALVES
        half = t % HALVES
        lanes = pl.ds(pl.multiple_of(half * half_width, half_width), half_width)
        q = qbuf[k, :, lanes]
        q = jnp.concatenate([q[:, h * HD:(h + 1) * HD] for h in range(PER_STEP)], axis=0)
        scaled = q.astype(F32) * (LOG2E / math.sqrt(HD))
        high = scaled.astype(BF16)
        low = (scaled - high.astype(F32)).astype(BF16)
        q = jnp.concatenate([high, low], axis=1)
        k_rows = win[pl.ds(lane + off(k), window_blocks), :, 0:HD].reshape(keys, HD)
        k_rows = jnp.concatenate([k_rows, k_rows], axis=1)
        sbuf[slot] = lax.dot_general(q, k_rows, (((1,), (1,)), ((), ())), preferred_element_type=F32)

    def soften(t, slot):
        r = lane + off(t // HALVES)
        scores = sbuf[slot].reshape(PER_STEP, rows, keys)
        scores = jnp.concatenate([
            scores[:, :, :first_edge] + bias[:, :rows][None],
            scores[:, :, first_edge:last_edge],
            scores[:, :, last_edge:] + bias[:, rows:][None],
        ], axis=2)
        top = jnp.max(scores, axis=-1, keepdims=True)
        weights = jnp.exp2(scores - top).astype(BF16)
        v_rows = win[pl.ds(r, window_blocks), :, HD:2 * HD].reshape(keys, HD)
        v_rows = jnp.concatenate([v_rows, ones[pl.ds(r, window_blocks)].reshape(keys, HD)], axis=1)
        weighted = jnp.dot(weights.reshape(PER_STEP * rows, keys), v_rows, preferred_element_type=F32)
        weighted = weighted[:, :HD] / weighted[:, HD:]
        wbuf[...] = weighted

    def rotate(t):
        k = t // HALVES
        half = t % HALVES
        signs = signs_buf[lane * HALVES + half].astype(F32)
        signed = wbuf[...].reshape(PER_STEP, rows, HD) * signs[:, None, :]
        signed = signed.reshape(PER_STEP * rows, HD)
        high = signed.astype(BF16)
        low = (signed - high.astype(F32)).astype(BF16)
        mixed = jnp.dot(high, had_ref[...], preferred_element_type=F32)
        mixed = mixed + jnp.dot(low, had_ref[...], preferred_element_type=F32)
        mixed = (mixed * (1.0 / math.sqrt(HD))).astype(BF16)
        start = lane * width + half * half_width
        for h in range(PER_STEP):
            rot[lane + off(k), :, pl.ds(pl.multiple_of(start + h * HD, HD), HD)] = mixed[h * rows:(h + 1) * rows]

    def step(t, slot):
        score(jnp.minimum(t + 1, STEPS - 1), 1 - slot)
        soften(t, slot)

        @pl.when(me < n)
        def _():
            rotate(t)

        @pl.when(t >= LAG)
        def _():
            rot_x_in(t - LAG).wait_recv()
            rot_f(t - LAG).start()

        for p in range(1, planes):
            @pl.when(t == due[p])
            def _():
                relay(p)

        rot_x(t).start()
        rot_c(t).start()

    def attend(k, carry):
        step(k * HALVES, 0)

        @pl.when(k < QUAD - 1)
        def _():
            remote(qbuf.at[k + 1], qbuf.at[k + 1], qs.at[k + 1], qr.at[k + 1], me + off(k + 1)).wait_recv()
        step(k * HALVES + 1, 1)
        return carry

    score(0, 0)
    lax.fori_loop(0, QUAD, attend, 0)
    def gathered(t, carry):
        rot_c_in(t).wait_recv()
        return carry

    def gathered_far(t, carry):
        rot_f_in(t).wait_recv()
        return carry

    lax.fori_loop(0, STEPS, gathered, 0)
    lax.fori_loop(0, STEPS // 2, gathered_far, 0)
    chunk_heads = 8
    words = GROUP // 8

    def lanes_of(unit, source_lane):
        s = unit * QUAD + source_lane
        return pl.ds(pl.multiple_of(s * cols, cols), cols)

    def out_send(unit, k):
        target = out_ref.at[:, lanes_of(unit, lane)]
        return remote(stage.at[unit, lane + off(k)], target, os.at[unit, k], orr.at[unit, k], me + off(k))

    def out_recv(unit, k):
        target = out_ref.at[:, lanes_of(unit, lane + off(k))]
        return remote(target, target, os.at[unit, k], orr.at[unit, k], me + off(k))

    def out_own(unit):
        return pltpu.make_async_copy(stage.at[unit, lane], out_ref.at[:, lanes_of(unit, lane)], ol.at[unit])

    def project(unit, side):
        scale = scales[:, lanes_of(unit, lane)]
        acc = jnp.zeros((2 * rows, cols), F32)
        for chunk in range(HEADS // chunk_heads):
            parts = []
            for h in range(chunk * chunk_heads, (chunk + 1) * chunk_heads):
                word = cbuf[unit, h * words:(h + 1) * words, :] ^ jnp.int32(-2004318072)
                factor = jnp.broadcast_to(scale[h:h + 1, :], (words, cols))
                for k in range(8):
                    code = jnp.right_shift(jnp.left_shift(word, 28 - 4 * k), 28)
                    parts.append(code.astype(F32).astype(BF16) * factor)
            weight = jnp.concatenate(parts, axis=0)
            span = chunk_heads * HD
            lhs = rot[pl.ds(2 * side, 2), :, chunk * span:(chunk + 1) * span].reshape(2 * rows, span)
            acc = acc + jnp.dot(lhs, weight, preferred_element_type=F32)
        stage[unit, pl.ds(2 * side, 2)] = acc.astype(BF16).reshape(2, rows, cols)

        @pl.when(side == x)
        def _():
            out_send(unit, 1).start()
            out_own(unit).start()

        @pl.when(side != x)
        def _():
            out_send(unit, 2).start()
            out_send(unit, 3).start()

    def sweep(i, carry):
        first = i < 2 * early
        rest = i - 2 * early
        q = jnp.where(first, i % early, early + rest // 2)
        partner = jnp.where(first, i < early, rest % 2 == 0)
        plane = plane_at(q // 2)
        other = q % 2

        for p in range(1, planes):
            @pl.when((i == item_due[p]) & (due[p] >= STEPS))
            def _():
                relay(p)

        @pl.when(i == early)
        def _():
            for t in range(STEPS - LAG, STEPS):
                rot_x_in(t).wait_recv()
                rot_f(t).start()
            lax.fori_loop(STEPS // 2, STEPS, gathered_far, 0)

        @pl.when(partner & (other == 1))
        def _():
            code_y_in(plane).wait_recv()

        project(plane * 2 + y + other * (1 - 2 * y), jnp.where(partner, 1 - x, x))
        return carry

    lax.fori_loop(0, 4 * planes, sweep, 0)

    for k in (1, 2, 3):
        kv_quad(k).wait_send()
        q_quad(k).wait_send()
    for slot in range(top_slot, -1, -2):
        for k in range(QUAD):
            forward_kv(slot, k, lambda copy: copy.wait_send())

    def drain_codes(k, carry):
        @pl.when((z - k >= 0) & has_up)
        def _():
            code_up(k).wait_send()

        @pl.when((z + k < planes) & has_down)
        def _():
            code_down(k).wait_send()
        code_y(k).wait_send()
        return carry

    lax.fori_loop(0, planes, drain_codes, 0)

    def drain_rot(t, carry):
        rot_x(t).wait_send()
        rot_c(t).wait_send()
        rot_f(t).wait_send()
        return carry

    lax.fori_loop(0, STEPS, drain_rot, 0)

    def drain_out(unit, carry):
        out_own(unit).wait()
        for k in (1, 2, 3):
            out_send(unit, k).wait_send()
            out_recv(unit, k).wait_recv()
        return carry

    lax.fori_loop(0, 2 * planes, drain_out, 0)


def on_device(queries, keys_values, head_signs, out_codes, out_scales):
    n = lax.axis_size("seq")
    rows = queries.shape[0]
    reach = (WINDOW + rows - 2) // rows
    span = -(-reach // QUAD)
    slots = span + 1
    assert slots % 2 == 1
    planes = n // (2 * QUAD)
    word_rows, cols = out_codes.shape
    vmem = pl.BlockSpec(memory_space=pltpu.VMEM)
    hbm = pl.BlockSpec(memory_space=pltpu.HBM)
    in_hbm = functools.partial(pltpu.with_memory_space_constraint, memory_space=pltpu.HBM)
    dma = pltpu.SemaphoreType.DMA
    per_head = keys_values.reshape(rows, 2, KV, HD).transpose(2, 0, 1, 3).reshape(KV, rows, 2 * HD)
    return pl.pallas_call(
        functools.partial(kernel, n, reach, slots),
        out_shape=pltpu.VMEM((rows, n * cols), BF16),
        in_specs=[hbm, vmem, hbm, vmem, hbm, hbm],
        out_specs=pl.BlockSpec(memory_space=pl.ANY),
        scratch_shapes=[
            pltpu.VMEM((slots * QUAD, rows, 2 * HD), BF16),
            pltpu.VMEM((slots * QUAD, rows, HD), BF16),
            pltpu.VMEM((QUAD, rows, LANE_HEADS * HD), BF16),
            pltpu.VMEM((2 * planes, word_rows, cols), jnp.int32),
            pltpu.VMEM((QUAD, rows, HEADS * HD), BF16),
            pltpu.VMEM((rows, 2 * rows), F32),
            pltpu.VMEM((2, PER_STEP * rows, (reach + 1) * rows), F32),
            pltpu.VMEM((PER_STEP * rows, HD), F32),
            pltpu.VMEM((2 * planes, QUAD, rows, cols), BF16),
            pltpu.VMEM((rows, HEADS * HD), BF16),
            pltpu.VMEM((STEPS, PER_STEP, HD), jnp.int32),
            pltpu.VMEM((HEADS, n * cols), BF16),
            dma((6,)),
            dma((QUAD,)), dma((QUAD,)),
            dma((QUAD,)), dma((QUAD,)),
            dma((slots // 2, QUAD)), dma((slots // 2, QUAD)),
            dma((slots // 2, QUAD)), dma((slots // 2, QUAD)),
            dma((planes + 1,)), dma((planes + 1,)),
            dma((planes + 1,)), dma((planes + 1,)),
            dma((planes,)), dma((planes,)),
            dma((STEPS,)), dma((STEPS,)),
            dma((STEPS,)), dma((STEPS,)),
            dma((STEPS,)), dma((STEPS,)),
            dma((2 * planes, QUAD)), dma((2 * planes, QUAD)),
            dma((2 * planes,)),
        ],
        compiler_params=pltpu.CompilerParams(
            collective_id=0, has_side_effects=True, vmem_limit_bytes=52 * 1000 * 1000
        ),
    )(
        in_hbm(queries),
        per_head,
        in_hbm(head_signs.reshape(STEPS, PER_STEP, HD)),
        reordered_hadamard(),
        in_hbm(out_codes),
        in_hbm(out_scales),
    )


def solution(mesh):
    return jax.shard_map(
        on_device,
        mesh=mesh,
        in_specs=(
            P(("groups", "seq"), None),
            P(("groups", "seq"), None, None),
            P(),
            P(None, "seq"),
            P(),
        ),
        out_specs=P(("groups", "seq"), None),
        check_vma=False,
    )
```

```python
import functools
import math

import jax
import jax.numpy as jnp
from jax import lax
from jax.experimental import pallas as pl
from jax.experimental.pallas import tpu as pltpu
from jax.sharding import PartitionSpec as P

HEADS = 32
KV = 4
HD = 128
GROUP = 128
WINDOW = 2048
QUAD = 4
LANE_HEADS = HEADS // QUAD
HALVES = 2
PER_STEP = LANE_HEADS // HALVES
STEPS = QUAD * HALVES
LAG = 5
LOG2E = 1.4426950408889634
MESH = pl.DeviceIdType.MESH
BF16 = jnp.bfloat16
F32 = jnp.float32


def reordered_hadamard():
    column = jnp.arange(HD, dtype=jnp.int32)
    source = (column % 16) * 8 + column // 16
    common = jnp.bitwise_and(jnp.arange(HD, dtype=jnp.int32)[:, None], source[None, :])
    ones = jnp.zeros((HD, HD), jnp.int32)
    for bit in range(HD.bit_length()):
        ones = ones + jnp.bitwise_and(jnp.right_shift(common, bit), 1)
    return jnp.where(ones % 2 == 0, 1.0, -1.0).astype(BF16)


def kernel(
    n, reach, slots,
    q_ref, kv_ref, sign_ref, had_ref, codes_ref, scales_ref, out_ref,
    win, ones, qbuf, cbuf, rot, bias, sbuf, wbuf, stage,
    q_all, signs_buf, scales, local_sem,
    kq_s, kq_r, qs, qr, zs, zr, ys, yr, up_s, up_r, dn_s, dn_r, cy_s, cy_r, cross_s, cross_r,
    rx_s, rx_r, rc_s, rc_r, rf_s, rf_r, os, orr, ol,
):
    rows = q_ref.shape[0]
    cols = codes_ref.shape[1]
    planes = n // (2 * QUAD)
    width = LANE_HEADS * HD
    half_width = PER_STEP * HD
    top_slot = slots - 1
    me = lax.axis_index("seq")
    z = me // (2 * QUAD)
    y = (me // QUAD) % 2
    lane = me % QUAD
    quad = me // QUAD
    core, x = lane % 2, lane // 2
    dc, dx, dy = 1 - 2 * core, 2 - 4 * x, QUAD - 2 * QUAD * y
    up, down = me + 2 * QUAD, me - 2 * QUAD
    has_up, has_down = z + 1 < planes, z >= 1

    def off(k):
        return (k % 2) * dc + (k // 2) * dx

    def remote(src, dst, send, recv, target):
        return pltpu.make_async_remote_copy(
            src_ref=src, dst_ref=dst, send_sem=send, recv_sem=recv,
            device_id={"seq": target}, device_id_type=MESH,
        )

    own_kv = pltpu.make_async_copy(
        kv_ref.at[lane], win.at[top_slot * QUAD + lane, :, pl.ds(0, 2 * HD)], local_sem.at[0])
    own_lanes = pl.ds(pl.multiple_of(lane * width, width), width)
    all_q = pltpu.make_async_copy(q_ref, q_all, local_sem.at[5])
    own_q = pltpu.make_async_copy(q_ref.at[:, own_lanes], qbuf.at[0], local_sem.at[1])
    own_codes = pltpu.make_async_copy(codes_ref, cbuf.at[quad], local_sem.at[2])
    all_signs = pltpu.make_async_copy(sign_ref, signs_buf, local_sem.at[3])
    all_scales = pltpu.make_async_copy(scales_ref, scales, local_sem.at[4])
    for copy in (own_kv, all_q, own_codes, own_q, all_signs, all_scales):
        copy.start()

    barrier = pltpu.get_barrier_semaphore()

    def greet(target):
        pl.semaphore_signal(barrier, inc=1, device_id={"seq": target}, device_id_type=MESH)

    for k in (2, 3, 1):
        greet(me + off(k))
    greet(me + dy)

    @pl.when(has_up)
    def _():
        greet(up)

    @pl.when(has_down)
    def _():
        greet(down)

    pl.semaphore_wait(barrier, QUAD + has_up.astype(jnp.int32) + has_down.astype(jnp.int32))

    def block(slot, k):
        return win.at[slot * QUAD + lane + off(k), :, pl.ds(0, 2 * HD)]

    def kv_quad(k):
        return remote(kv_ref.at[lane + off(k)], win.at[top_slot * QUAD + lane, :, pl.ds(0, 2 * HD)],
                      kq_s.at[k], kq_r.at[k], me + off(k))

    def kv_quad_in(k):
        return remote(block(top_slot, k), block(top_slot, k), kq_s.at[k], kq_r.at[k], me + off(k))

    def source(slot, k):
        return kv_ref.at[lane] if slot == top_slot and k == 0 else block(slot, k)

    def z_kv(slot, k):
        return remote(source(slot, k), block(slot - 2, k),
                      zs.at[(top_slot - slot) // 2, k], zr.at[(top_slot - slot) // 2, k], up)

    def y_kv(slot, target, k):
        level = (top_slot - 1 - target) // 2
        return remote(source(slot, k), block(target, k), ys.at[level, k], yr.at[level, k], me + dy)

    def there(slot):
        return quad - top_slot + slot >= 0

    def forward_kv(slot, k, act):
        if slot >= 2:
            @pl.when(there(slot) & has_up)
            def _():
                act(z_kv(slot, k))
        if slot >= 1:
            @pl.when(there(slot) & (y == 0))
            def _():
                act(y_kv(slot, slot - 1, k))
        if slot + 1 < top_slot:
            @pl.when(there(slot) & (y == 1))
            def _():
                act(y_kv(slot, slot + 1, k))

    def q_quad(k):
        lanes = pl.ds(pl.multiple_of((lane + off(k)) * width, width), width)
        return remote(q_all.at[:, lanes], qbuf.at[k], qs.at[k], qr.at[k], me + off(k))

    def code_up(k):
        unit = cbuf.at[quad - 2 * k]
        return remote(unit, unit, up_s.at[k + 1], up_r.at[k + 1], up)

    def code_up_in(k):
        unit = cbuf.at[quad - 2 * k]
        return remote(unit, unit, up_s.at[k], up_r.at[k], up)

    def code_down(k):
        unit = cbuf.at[quad + 2 * k]
        return remote(unit, unit, dn_s.at[k + 1], dn_r.at[k + 1], down)

    def code_down_in(k):
        unit = cbuf.at[quad + 2 * k]
        return remote(unit, unit, dn_s.at[k], dn_r.at[k], down)

    half_words = cbuf.shape[1] // 2

    def far(plane):
        return ((plane == 0) | (plane == planes - 1)) & (plane != z)

    def each_y(plane, column, act):
        def copy(unit):
            return remote(unit, unit, cy_s.at[plane], cy_r.at[plane], me + dy)

        @pl.when(far(plane))
        def _():
            act(copy(cbuf.at[plane * 2 + column, pl.ds(0, half_words)]))

        @pl.when(jnp.logical_not(far(plane)))
        def _():
            act(copy(cbuf.at[plane * 2 + column]))

    def send_y(plane):
        each_y(plane, y, lambda copy: copy.start())

    def wait_y(plane):
        each_y(plane, 1 - y, lambda copy: copy.wait_recv())

    def cross_up():
        unit = cbuf.at[1 - y, pl.ds(half_words, half_words)]
        return remote(unit, unit, cross_s.at[0], cross_r.at[0], up)

    def cross_down():
        unit = cbuf.at[(planes - 1) * 2 + 1 - y, pl.ds(half_words, half_words)]
        return remote(unit, unit, cross_s.at[1], cross_r.at[1], down)

    near = jnp.minimum(z, planes - 1 - z)
    toward = jnp.where(z <= planes - 1 - z, 1, -1)

    def plane_at(p):
        both = z + ((p + 1) // 2) * (2 * (p % 2) - 1)
        return jnp.where(p <= 2 * near, both, z + toward * (p - near))

    early = planes + 1

    def relay(p):
        plane = plane_at(p)

        @pl.when(plane < z)
        def _():
            code_up_in(z - plane).wait_recv()

            @pl.when(has_up)
            def _():
                code_up(z - plane).start()
            send_y(plane)

        @pl.when(plane > z)
        def _():
            code_down_in(plane - z).wait_recv()

            @pl.when(has_down)
            def _():
                code_down(plane - z).start()
            send_y(plane)

    def own_y():
        wait_y(z)

        @pl.when((z == 0) & has_up)
        def _():
            cross_up().start()

        @pl.when((z == planes - 1) & has_down)
        def _():
            cross_down().start()

    def relay_cross_up():
        @pl.when(has_down)
        def _():
            cross_up().wait_recv()

            @pl.when(has_up)
            def _():
                cross_up().start()

    def relay_cross_down():
        @pl.when(has_up)
        def _():
            cross_down().wait_recv()

            @pl.when(has_down)
            def _():
                cross_down().start()

    begin = jnp.where(z == 0, 80, jnp.where(z == 1, 138, 165))
    after = begin + 19 * STEPS + 15

    def item_of(q):
        return STEPS + jnp.where(q < early, q, 2 * early + 2 * (q - early))

    events = []

    def expect(action, arrival, deadline, prologue=None):
        step_at = jnp.clip((arrival - begin - 10) // 20, 0, STEPS - 1)
        item_at = STEPS + jnp.maximum(arrival - after, 0) // 9
        at = jnp.minimum(jnp.where(arrival < after, step_at, item_at), deadline)
        if prologue is not None:
            at = jnp.where(prologue, -1, at)
        events.append((action, arrival, at))

    for p in range(1, planes):
        d = plane_at(p) - z
        arrival = jnp.where(d > 0, 130 * d, jnp.where(z == 1, 71, 130) - 117 * d)
        expect(functools.partial(relay, p), arrival, item_of(2 * p - 1), (d == 1) & has_down)
    expect(own_y, jnp.where(z == 0, 185, jnp.where(z == 1, 255, 290)), item_of(1))
    bottom = jnp.where(z == near, 2 * z, planes - 1)
    top_at = jnp.where(planes - 1 - z == near, 2 * near - 1, planes - 1)
    expect(relay_cross_up, jnp.where(z == 1, 275, 170 + 130 * z), item_of(2 * bottom + 1))
    expect(relay_cross_down, 290 + 71 * (planes - 1 - z), item_of(2 * jnp.maximum(top_at, 0) + 1))
    timed = []
    for action, arrival, _ in events:
        at = None
        for _, other_arrival, other_at in events:
            later = jnp.where(other_arrival >= arrival, other_at, STEPS + 4 * planes)
            at = later if at is None else jnp.minimum(at, later)
        timed.append((action, at))

    def run_events(now):
        for action, at in timed:
            pl.when(at == now)(action)

    for k in (2, 3, 1):
        kv_quad(k).start()
    forward_kv(top_slot, 0, lambda copy: copy.start())

    own_codes.wait()

    @pl.when(has_down)
    def _():
        code_down(0).start()
    all_q.wait()
    for k in (1, 2, 3):
        q_quad(k).start()

    window_blocks = reach + 1
    keys = window_blocks * rows
    for edge, offset in ((0, reach * rows), (1, 0)):
        query = lax.broadcasted_iota(jnp.int32, (rows, rows), 0)
        key = lax.broadcasted_iota(jnp.int32, (rows, rows), 1) - offset
        gap = query - key
        bias[:, edge * rows:(edge + 1) * rows] = jnp.where((gap >= 0) & (gap < WINDOW), 0.0, -jnp.inf).astype(F32)
    for slot in range(slots):
        value = jnp.where(there(slot), 1.0, 0.0).astype(F32)
        ones[slot * QUAD:(slot + 1) * QUAD] = jnp.full((QUAD, rows, HD), value, F32).astype(BF16)

    def take_quad(k):
        kv_quad_in(k).wait_recv()
        forward_kv(top_slot, k, lambda copy: copy.start())

    def take_z(slot, k):
        @pl.when(there(slot))
        def _():
            z_kv(slot + 2, k).wait_recv()
        forward_kv(slot, k, lambda copy: copy.start())

    levels = range(top_slot - 2, -1, -2)
    take_quad(1)
    own_kv.wait()
    take_z(top_slot - 2, 0)
    take_z(top_slot - 2, 1)
    take_quad(2)
    take_quad(3)
    for slot in levels[1:]:
        take_z(slot, 0)
        take_z(slot, 1)
    take_z(top_slot - 2, 2)
    take_z(top_slot - 2, 3)

    @pl.when(has_up)
    def _():
        code_up(0).start()

    @pl.when(y == 0)
    def _():
        send_y(z)
    for slot in levels[1:]:
        take_z(slot, 2)
        take_z(slot, 3)

    @pl.when(y == 1)
    def _():
        send_y(z)

    run_events(-1)
    for slot in range(top_slot):
        @pl.when(jnp.logical_not(there(slot)))
        def _():
            first = win[top_slot * QUAD, 0:1, 0:HD].astype(F32)
            fill = jnp.concatenate([jnp.broadcast_to(first, (rows, HD)), jnp.zeros((rows, HD), F32)], axis=1)
            fill = fill.astype(BF16)
            for i in range(QUAD):
                win[slot * QUAD + i] = fill

    for slot in range(top_slot - 1, -1, -2):
        for k in range(QUAD):
            @pl.when(there(slot))
            def _():
                level = (top_slot - 1 - slot) // 2
                remote(block(slot, k), block(slot, k), ys.at[level, k], yr.at[level, k], me + dy).wait_recv()
    own_q.wait()
    all_signs.wait()
    all_scales.wait()

    def piece(r, source_lane, half):
        start = source_lane * width + half * half_width
        return rot.at[r, :, pl.ds(pl.multiple_of(start, half_width), half_width)]

    def rot_x(t):
        ref = piece(lane + off(t // 2), lane, t % 2)
        return remote(ref, ref, rx_s.at[t], rx_r.at[t], me + dx)

    def rot_c(t):
        ref = piece(lane + off(t // 2), lane, t % 2)
        return remote(ref, ref, rc_s.at[t], rc_r.at[t], me + dc)

    def rot_x_in(t):
        k = t // 2
        ref = piece(lane + dx + (k % 2) * dc - (k // 2) * dx, lane + dx, t % 2)
        return remote(ref, ref, rx_s.at[t], rx_r.at[t], me + dx)

    def rot_f(t):
        k = t // 2
        ref = piece(lane + dx + (k % 2) * dc - (k // 2) * dx, lane + dx, t % 2)
        return remote(ref, ref, rf_s.at[t], rf_r.at[t], me + dc)

    def rot_c_in(t):
        k = t // 2
        ref = piece(lane + dc - (k % 2) * dc + (k // 2) * dx, lane + dc, t % 2)
        return remote(ref, ref, rc_s.at[t], rc_r.at[t], me + dc)

    def rot_f_in(t):
        k = t // 2
        ref = piece(lane + dc + dx - (k % 2) * dc - (k // 2) * dx, lane + dc + dx, t % 2)
        return remote(ref, ref, rf_s.at[t], rf_r.at[t], me + dc)

    first_edge, last_edge = rows, keys - rows

    def score(t, slot):
        k = t // HALVES
        half = t % HALVES
        lanes = pl.ds(pl.multiple_of(half * half_width, half_width), half_width)
        q = qbuf[k, :, lanes]
        q = jnp.concatenate([q[:, h * HD:(h + 1) * HD] for h in range(PER_STEP)], axis=0)
        scaled = q.astype(F32) * (LOG2E / math.sqrt(HD))
        high = scaled.astype(BF16)
        low = (scaled - high.astype(F32)).astype(BF16)
        q = jnp.concatenate([high, low], axis=1)
        k_rows = win[pl.ds(lane + off(k), window_blocks), :, 0:HD].reshape(keys, HD)
        k_rows = jnp.concatenate([k_rows, k_rows], axis=1)
        sbuf[slot] = lax.dot_general(q, k_rows, (((1,), (1,)), ((), ())), preferred_element_type=F32)

    def soften(t, slot):
        r = lane + off(t // HALVES)
        scores = sbuf[slot].reshape(PER_STEP, rows, keys)
        scores = jnp.concatenate([
            scores[:, :, :first_edge] + bias[:, :rows][None],
            scores[:, :, first_edge:last_edge],
            scores[:, :, last_edge:] + bias[:, rows:][None],
        ], axis=2)
        top = jnp.max(scores, axis=-1, keepdims=True)
        weights = jnp.exp2(scores - top).astype(BF16)
        v_rows = win[pl.ds(r, window_blocks), :, HD:2 * HD].reshape(keys, HD)
        v_rows = jnp.concatenate([v_rows, ones[pl.ds(r, window_blocks)].reshape(keys, HD)], axis=1)
        weighted = jnp.dot(weights.reshape(PER_STEP * rows, keys), v_rows, preferred_element_type=F32)
        weighted = weighted[:, :HD] / weighted[:, HD:]
        wbuf[...] = weighted

    def rotate(t):
        k = t // HALVES
        half = t % HALVES
        signs = signs_buf[lane * HALVES + half].astype(F32)
        signed = wbuf[...].reshape(PER_STEP, rows, HD) * signs[:, None, :]
        signed = signed.reshape(PER_STEP * rows, HD)
        high = signed.astype(BF16)
        low = (signed - high.astype(F32)).astype(BF16)
        mixed = jnp.dot(high, had_ref[...], preferred_element_type=F32)
        mixed = mixed + jnp.dot(low, had_ref[...], preferred_element_type=F32)
        mixed = (mixed * (1.0 / math.sqrt(HD))).astype(BF16)
        start = lane * width + half * half_width
        for h in range(PER_STEP):
            rot[lane + off(k), :, pl.ds(pl.multiple_of(start + h * HD, HD), HD)] = mixed[h * rows:(h + 1) * rows]

    def step(t, slot):
        score(jnp.minimum(t + 1, STEPS - 1), 1 - slot)
        soften(t, slot)

        @pl.when(me < n)
        def _():
            rotate(t)

        @pl.when(t >= LAG)
        def _():
            rot_x_in(t - LAG).wait_recv()
            rot_f(t - LAG).start()

        run_events(t)
        rot_x(t).start()
        rot_c(t).start()

    def attend(k, carry):
        step(k * HALVES, 0)

        @pl.when(k < QUAD - 1)
        def _():
            remote(qbuf.at[k + 1], qbuf.at[k + 1], qs.at[k + 1], qr.at[k + 1], me + off(k + 1)).wait_recv()
        step(k * HALVES + 1, 1)
        return carry

    score(0, 0)
    lax.fori_loop(0, QUAD, attend, 0)
    for t in range(STEPS - LAG, STEPS // 2):
        rot_x_in(t).wait_recv()
        rot_f(t).start()

    def gathered(t, carry):
        rot_c_in(t).wait_recv()
        return carry

    def gathered_far(t, carry):
        rot_f_in(t).wait_recv()
        return carry

    lax.fori_loop(0, STEPS, gathered, 0)
    lax.fori_loop(0, STEPS // 2, gathered_far, 0)
    chunk_heads = 8
    words = GROUP // 8

    def lanes_of(unit, source_lane):
        s = unit * QUAD + source_lane
        return pl.ds(pl.multiple_of(s * cols, cols), cols)

    def out_send(unit, k):
        target = out_ref.at[:, lanes_of(unit, lane)]
        return remote(stage.at[unit, lane + off(k)], target, os.at[unit, k], orr.at[unit, k], me + off(k))

    def out_recv(unit, k):
        target = out_ref.at[:, lanes_of(unit, lane + off(k))]
        return remote(target, target, os.at[unit, k], orr.at[unit, k], me + off(k))

    def out_own(unit):
        return pltpu.make_async_copy(stage.at[unit, lane], out_ref.at[:, lanes_of(unit, lane)], ol.at[unit])

    def project(unit, side):
        scale = scales[:, lanes_of(unit, lane)]
        acc = jnp.zeros((2 * rows, cols), F32)
        for chunk in range(HEADS // chunk_heads):
            parts = []
            for h in range(chunk * chunk_heads, (chunk + 1) * chunk_heads):
                word = cbuf[unit, h * words:(h + 1) * words, :] ^ jnp.int32(-2004318072)
                factor = jnp.broadcast_to(scale[h:h + 1, :], (words, cols))
                for k in range(8):
                    code = jnp.right_shift(jnp.left_shift(word, 28 - 4 * k), 28)
                    parts.append(code.astype(F32).astype(BF16) * factor)
            weight = jnp.concatenate(parts, axis=0)
            span = chunk_heads * HD
            lhs = rot[pl.ds(2 * side, 2), :, chunk * span:(chunk + 1) * span].reshape(2 * rows, span)
            acc = acc + jnp.dot(lhs, weight, preferred_element_type=F32)
        stage[unit, pl.ds(2 * side, 2)] = acc.astype(BF16).reshape(2, rows, cols)

        @pl.when(side == x)
        def _():
            out_send(unit, 1).start()
            out_own(unit).start()

        @pl.when(side != x)
        def _():
            out_send(unit, 2).start()
            out_send(unit, 3).start()

    def sweep(i, carry):
        first = i < 2 * early
        rest = i - 2 * early
        q = jnp.where(first, i % early, early + rest // 2)
        partner = jnp.where(first, i < early, rest % 2 == 0)
        plane = plane_at(q // 2)
        other = q % 2

        run_events(STEPS + i)

        @pl.when(i == early)
        def _():
            for t in range(max(STEPS - LAG, STEPS // 2), STEPS):
                rot_x_in(t).wait_recv()
                rot_f(t).start()
            lax.fori_loop(STEPS // 2, STEPS, gathered_far, 0)

        @pl.when(partner & (other == 1) & (plane != z))
        def _():
            wait_y(plane)

        project(plane * 2 + y + other * (1 - 2 * y), jnp.where(partner, 1 - x, x))
        return carry

    lax.fori_loop(0, 4 * planes, sweep, 0)

    for k in (1, 2, 3):
        kv_quad(k).wait_send()
        q_quad(k).wait_send()
    for slot in range(top_slot, -1, -2):
        for k in range(QUAD):
            forward_kv(slot, k, lambda copy: copy.wait_send())

    def drain_codes(k, carry):
        @pl.when((z - k >= 0) & has_up)
        def _():
            code_up(k).wait_send()

        @pl.when((z + k < planes) & has_down)
        def _():
            code_down(k).wait_send()
        each_y(k, y, lambda copy: copy.wait_send())
        return carry

    lax.fori_loop(0, planes, drain_codes, 0)

    @pl.when(has_up)
    def _():
        cross_up().wait_send()

    @pl.when(has_down)
    def _():
        cross_down().wait_send()

    def drain_rot(t, carry):
        rot_x(t).wait_send()
        rot_c(t).wait_send()
        rot_f(t).wait_send()
        return carry

    lax.fori_loop(0, STEPS, drain_rot, 0)

    def drain_out(unit, carry):
        out_own(unit).wait()
        for k in (1, 2, 3):
            out_send(unit, k).wait_send()
            out_recv(unit, k).wait_recv()
        return carry

    lax.fori_loop(0, 2 * planes, drain_out, 0)


def on_device(queries, keys_values, head_signs, out_codes, out_scales):
    n = lax.axis_size("seq")
    rows = queries.shape[0]
    reach = (WINDOW + rows - 2) // rows
    span = -(-reach // QUAD)
    slots = span + 1
    assert slots % 2 == 1
    planes = n // (2 * QUAD)
    word_rows, cols = out_codes.shape
    vmem = pl.BlockSpec(memory_space=pltpu.VMEM)
    hbm = pl.BlockSpec(memory_space=pltpu.HBM)
    in_hbm = functools.partial(pltpu.with_memory_space_constraint, memory_space=pltpu.HBM)
    dma = pltpu.SemaphoreType.DMA
    per_head = keys_values.reshape(rows, 2, KV, HD).transpose(2, 0, 1, 3).reshape(KV, rows, 2 * HD)
    return pl.pallas_call(
        functools.partial(kernel, n, reach, slots),
        out_shape=pltpu.VMEM((rows, n * cols), BF16),
        in_specs=[hbm, vmem, hbm, vmem, hbm, hbm],
        out_specs=pl.BlockSpec(memory_space=pl.ANY),
        scratch_shapes=[
            pltpu.VMEM((slots * QUAD, rows, 2 * HD), BF16),
            pltpu.VMEM((slots * QUAD, rows, HD), BF16),
            pltpu.VMEM((QUAD, rows, LANE_HEADS * HD), BF16),
            pltpu.VMEM((2 * planes, word_rows, cols), jnp.int32),
            pltpu.VMEM((QUAD, rows, HEADS * HD), BF16),
            pltpu.VMEM((rows, 2 * rows), F32),
            pltpu.VMEM((2, PER_STEP * rows, (reach + 1) * rows), F32),
            pltpu.VMEM((PER_STEP * rows, HD), F32),
            pltpu.VMEM((2 * planes, QUAD, rows, cols), BF16),
            pltpu.VMEM((rows, HEADS * HD), BF16),
            pltpu.VMEM((STEPS, PER_STEP, HD), jnp.int32),
            pltpu.VMEM((HEADS, n * cols), BF16),
            dma((6,)),
            dma((QUAD,)), dma((QUAD,)),
            dma((QUAD,)), dma((QUAD,)),
            dma((slots // 2, QUAD)), dma((slots // 2, QUAD)),
            dma((slots // 2, QUAD)), dma((slots // 2, QUAD)),
            dma((planes + 1,)), dma((planes + 1,)),
            dma((planes + 1,)), dma((planes + 1,)),
            dma((planes,)), dma((planes,)),
            dma((2,)), dma((2,)),
            dma((STEPS,)), dma((STEPS,)),
            dma((STEPS,)), dma((STEPS,)),
            dma((STEPS,)), dma((STEPS,)),
            dma((2 * planes, QUAD)), dma((2 * planes, QUAD)),
            dma((2 * planes,)),
        ],
        compiler_params=pltpu.CompilerParams(
            collective_id=0, has_side_effects=True, vmem_limit_bytes=52 * 1000 * 1000
        ),
    )(
        in_hbm(queries),
        per_head,
        in_hbm(head_signs.reshape(STEPS, PER_STEP, HD)),
        reordered_hadamard(),
        in_hbm(out_codes),
        in_hbm(out_scales),
    )


def solution(mesh):
    return jax.shard_map(
        on_device,
        mesh=mesh,
        in_specs=(
            P(("groups", "seq"), None),
            P(("groups", "seq"), None, None),
            P(),
            P(None, "seq"),
            P(),
        ),
        out_specs=P(("groups", "seq"), None),
        check_vma=False,
    )
```

```python
import functools
import math

import jax
import jax.numpy as jnp
from jax import lax
from jax.experimental import pallas as pl
from jax.experimental.pallas import tpu as pltpu
from jax.sharding import PartitionSpec as P

HEADS = 32
KV = 4
HD = 128
GROUP = 128
WINDOW = 2048
QUAD = 4
LANE_HEADS = HEADS // QUAD
HALVES = 2
PER_STEP = LANE_HEADS // HALVES
STEPS = QUAD * HALVES
LAG = 5
LOG2E = 1.4426950408889634
MESH = pl.DeviceIdType.MESH
BF16 = jnp.bfloat16
F32 = jnp.float32


def reordered_hadamard():
    column = jnp.arange(HD, dtype=jnp.int32)
    source = (column % 16) * 8 + column // 16
    common = jnp.bitwise_and(jnp.arange(HD, dtype=jnp.int32)[:, None], source[None, :])
    ones = jnp.zeros((HD, HD), jnp.int32)
    for bit in range(HD.bit_length()):
        ones = ones + jnp.bitwise_and(jnp.right_shift(common, bit), 1)
    return jnp.where(ones % 2 == 0, 1.0, -1.0).astype(BF16)


def kernel(
    n, reach, slots,
    q_ref, kv_ref, sign_ref, had_ref, codes_ref, scales_ref, out_ref,
    win, ones, qbuf, cbuf, rot, bias, sbuf, wbuf, tops, sums, stage,
    q_all, signs_buf, scales, kv_raw, kv_heads, local_sem,
    kq_s, kq_r, qs, qr, zs, zr, ys, yr, up_s, up_r, dn_s, dn_r, cy_s, cy_r, cross_s, cross_r,
    rx_s, rx_r, rc_s, rc_r, rf_s, rf_r, os, orr, ol,
):
    rows = q_ref.shape[0]
    cols = codes_ref.shape[1]
    planes = n // (2 * QUAD)
    width = LANE_HEADS * HD
    half_width = PER_STEP * HD
    top_slot = slots - 1
    me = lax.axis_index("seq")
    z = me // (2 * QUAD)
    y = (me // QUAD) % 2
    lane = me % QUAD
    quad = me // QUAD
    core, x = lane % 2, lane // 2
    dc, dx, dy = 1 - 2 * core, 2 - 4 * x, QUAD - 2 * QUAD * y
    up, down = me + 2 * QUAD, me - 2 * QUAD
    has_up, has_down = z + 1 < planes, z >= 1

    def off(k):
        return (k % 2) * dc + (k // 2) * dx

    def remote(src, dst, send, recv, target):
        return pltpu.make_async_remote_copy(
            src_ref=src, dst_ref=dst, send_sem=send, recv_sem=recv,
            device_id={"seq": target}, device_id_type=MESH,
        )

    window_blocks = reach + 1
    keys = window_blocks * rows
    raw_kv = pltpu.make_async_copy(kv_ref, kv_raw, local_sem.at[6])
    own_kv = pltpu.make_async_copy(
        kv_heads.at[lane], win.at[top_slot * QUAD + lane, :, pl.ds(0, 2 * HD)], local_sem.at[0])
    own_lanes = pl.ds(pl.multiple_of(lane * width, width), width)
    all_q = pltpu.make_async_copy(q_ref, q_all, local_sem.at[5])
    own_q = pltpu.make_async_copy(q_ref.at[:, own_lanes], qbuf.at[0], local_sem.at[1])
    own_codes = pltpu.make_async_copy(codes_ref, cbuf.at[quad], local_sem.at[2])
    all_signs = pltpu.make_async_copy(sign_ref, signs_buf, local_sem.at[3])
    all_scales = pltpu.make_async_copy(scales_ref, scales, local_sem.at[4])
    for copy in (raw_kv, all_q, own_codes, own_q, all_signs, all_scales):
        copy.start()

    barrier = pltpu.get_barrier_semaphore()

    def greet(target):
        pl.semaphore_signal(barrier, inc=1, device_id={"seq": target}, device_id_type=MESH)

    for k in (2, 3, 1):
        greet(me + off(k))
    greet(me + dy)

    @pl.when(has_up)
    def _():
        greet(up)

    @pl.when(has_down)
    def _():
        greet(down)

    raw_kv.wait()
    pairs = kv_raw[...].reshape(2 * rows, KV * HD)
    to = lax.broadcasted_iota(jnp.int32, (rows, 2 * rows), 0)
    source_row = lax.broadcasted_iota(jnp.int32, (rows, 2 * rows), 1)
    for which in range(2):
        pick = jnp.where(source_row == 2 * to + which, 1.0, 0.0).astype(BF16)
        picked = jnp.dot(pick, pairs, preferred_element_type=F32).astype(BF16)
        for g in range(KV):
            kv_heads[g, :, which * HD:(which + 1) * HD] = picked[:, g * HD:(g + 1) * HD]
    pl.semaphore_wait(barrier, QUAD + has_up.astype(jnp.int32) + has_down.astype(jnp.int32))

    own_kv.start()
    def block(slot, k):
        return win.at[slot * QUAD + lane + off(k), :, pl.ds(0, 2 * HD)]

    def kv_quad(k):
        return remote(kv_heads.at[lane + off(k)], win.at[top_slot * QUAD + lane, :, pl.ds(0, 2 * HD)],
                      kq_s.at[k], kq_r.at[k], me + off(k))

    def kv_quad_in(k):
        return remote(block(top_slot, k), block(top_slot, k), kq_s.at[k], kq_r.at[k], me + off(k))

    def source(slot, k):
        return kv_heads.at[lane] if slot == top_slot and k == 0 else block(slot, k)

    def z_kv(slot, k):
        return remote(source(slot, k), block(slot - 2, k),
                      zs.at[(top_slot - slot) // 2, k], zr.at[(top_slot - slot) // 2, k], up)

    def y_kv(slot, target, k):
        level = (top_slot - 1 - target) // 2
        return remote(source(slot, k), block(target, k), ys.at[level, k], yr.at[level, k], me + dy)

    def there(slot):
        return quad - top_slot + slot >= 0

    def forward_kv(slot, k, act):
        if slot >= 2:
            @pl.when(there(slot) & has_up)
            def _():
                act(z_kv(slot, k))
        if slot >= 1:
            @pl.when(there(slot) & (y == 0))
            def _():
                act(y_kv(slot, slot - 1, k))
        if slot + 1 < top_slot:
            @pl.when(there(slot) & (y == 1))
            def _():
                act(y_kv(slot, slot + 1, k))

    def q_quad(k):
        lanes = pl.ds(pl.multiple_of((lane + off(k)) * width, width), width)
        return remote(q_all.at[:, lanes], qbuf.at[k], qs.at[k], qr.at[k], me + off(k))

    def code_up(k):
        unit = cbuf.at[quad - 2 * k]
        return remote(unit, unit, up_s.at[k + 1], up_r.at[k + 1], up)

    def code_up_in(k):
        unit = cbuf.at[quad - 2 * k]
        return remote(unit, unit, up_s.at[k], up_r.at[k], up)

    def code_down(k):
        unit = cbuf.at[quad + 2 * k]
        return remote(unit, unit, dn_s.at[k + 1], dn_r.at[k + 1], down)

    def code_down_in(k):
        unit = cbuf.at[quad + 2 * k]
        return remote(unit, unit, dn_s.at[k], dn_r.at[k], down)

    half_words = cbuf.shape[1] // 2

    def far(plane):
        return ((plane == 0) | (plane == planes - 1)) & (plane != z)

    def each_y(plane, column, act):
        def copy(unit):
            return remote(unit, unit, cy_s.at[plane], cy_r.at[plane], me + dy)

        @pl.when(far(plane))
        def _():
            act(copy(cbuf.at[plane * 2 + column, pl.ds(0, half_words)]))

        @pl.when(jnp.logical_not(far(plane)))
        def _():
            act(copy(cbuf.at[plane * 2 + column]))

    def send_y(plane):
        each_y(plane, y, lambda copy: copy.start())

    def wait_y(plane):
        each_y(plane, 1 - y, lambda copy: copy.wait_recv())

    def cross_up():
        unit = cbuf.at[1 - y, pl.ds(half_words, half_words)]
        return remote(unit, unit, cross_s.at[0], cross_r.at[0], up)

    def cross_down():
        unit = cbuf.at[(planes - 1) * 2 + 1 - y, pl.ds(half_words, half_words)]
        return remote(unit, unit, cross_s.at[1], cross_r.at[1], down)

    near = jnp.minimum(z, planes - 1 - z)
    toward = jnp.where(z <= planes - 1 - z, 1, -1)

    def plane_at(p):
        both = z + ((p + 1) // 2) * (2 * (p % 2) - 1)
        return jnp.where(p <= 2 * near, both, z + toward * (p - near))

    early = planes + 1

    def relay(p):
        plane = plane_at(p)

        @pl.when(plane < z)
        def _():
            code_up_in(z - plane).wait_recv()

            @pl.when(has_up)
            def _():
                code_up(z - plane).start()
            send_y(plane)

        @pl.when(plane > z)
        def _():
            code_down_in(plane - z).wait_recv()

            @pl.when(has_down)
            def _():
                code_down(plane - z).start()
            send_y(plane)

    def own_y():
        wait_y(z)

        @pl.when((z == 0) & has_up)
        def _():
            cross_up().start()

        @pl.when((z == planes - 1) & has_down)
        def _():
            cross_down().start()

    def relay_cross_up():
        @pl.when(has_down)
        def _():
            cross_up().wait_recv()

            @pl.when(has_up)
            def _():
                cross_up().start()

    def relay_cross_down():
        @pl.when(has_up)
        def _():
            cross_down().wait_recv()

            @pl.when(has_down)
            def _():
                cross_down().start()

    begin = jnp.where(z == 0, 80, jnp.where(z == 1, 138, 165))
    after = jnp.where(z == 0, 295, jnp.where(z == 1, 318, 335))
    stall = 55

    def item_of(q):
        return STEPS + jnp.where(q < early, q, 2 * early + 2 * (q - early))

    events = []

    def expect(action, arrival, deadline, prologue=None):
        step_at = jnp.clip((arrival - begin - 10) // 20, 0, STEPS - 1)
        wait = arrival - after
        later = early + jnp.maximum(wait - 9 * early - stall, 0) // 9
        item_at = STEPS + jnp.where(wait < 9 * early, wait // 9, later)
        at = jnp.minimum(jnp.where(arrival < after, step_at, item_at), deadline)
        if prologue is not None:
            at = jnp.where(prologue, -1, at)
        events.append((action, arrival, at))

    for p in range(1, planes):
        d = plane_at(p) - z
        arrival = jnp.where(d > 0, 130 * d, jnp.where(z == 1, 71, 130) - 117 * d)
        expect(functools.partial(relay, p), arrival, item_of(2 * p - 1), (d == 1) & has_down)
    expect(own_y, jnp.where(z == 0, 185, jnp.where(z == 1, 255, 290)), item_of(1))
    bottom = jnp.where(z == near, 2 * z, planes - 1)
    top_at = jnp.where(planes - 1 - z == near, 2 * near - 1, planes - 1)
    expect(relay_cross_up, jnp.where(z == 1, 275, 170 + 130 * z), item_of(2 * bottom + 1))
    expect(relay_cross_down, 290 + 71 * (planes - 1 - z), item_of(2 * jnp.maximum(top_at, 0) + 1))
    timed = []
    for action, arrival, _ in events:
        at = None
        for _, other_arrival, other_at in events:
            later = jnp.where(other_arrival >= arrival, other_at, STEPS + 4 * planes)
            at = later if at is None else jnp.minimum(at, later)
        timed.append((action, at))

    def run_events(now):
        for action, at in timed:
            pl.when(at == now)(action)

    def score(t, slot, first=0, count=None):
        count = window_blocks if count is None else count
        k = t // HALVES
        half = t % HALVES
        lanes = pl.ds(pl.multiple_of(half * half_width, half_width), half_width)
        q = qbuf[k, :, lanes]
        q = jnp.concatenate([q[:, h * HD:(h + 1) * HD] for h in range(PER_STEP)], axis=0)
        scaled = q.astype(F32) * (LOG2E / math.sqrt(HD))
        high = scaled.astype(BF16)
        low = (scaled - high.astype(F32)).astype(BF16)
        q = jnp.concatenate([high, low], axis=1)
        k_rows = win[pl.ds(lane + off(k) + first, count), :, 0:HD].reshape(count * rows, HD)
        k_rows = jnp.concatenate([k_rows, k_rows], axis=1)
        part = lax.dot_general(q, k_rows, (((1,), (1,)), ((), ())), preferred_element_type=F32)
        sbuf[slot, :, first * rows:(first + count) * rows] = part

    def soft_part(slot, r, first, count):
        scores = sbuf[slot, :, first * rows:(first + count) * rows].reshape(PER_STEP, rows, count * rows)
        head, tail = rows if first == 0 else 0, rows if first + count == window_blocks else 0
        parts = [scores[:, :, head:count * rows - tail]]
        if head:
            parts.insert(0, scores[:, :, :head] + bias[:, :rows][None])
        if tail:
            parts.append(scores[:, :, count * rows - tail:] + bias[:, rows:][None])
        scores = jnp.concatenate(parts, axis=2)
        top = jnp.max(scores, axis=-1, keepdims=True)
        weights = jnp.exp2(scores - top).astype(BF16)
        v_rows = win[pl.ds(r + first, count), :, HD:2 * HD].reshape(count * rows, HD)
        v_rows = jnp.concatenate([v_rows, ones[pl.ds(r + first, count)].reshape(count * rows, HD)], axis=1)
        weighted = jnp.dot(weights.reshape(PER_STEP * rows, count * rows), v_rows, preferred_element_type=F32)
        return top.reshape(PER_STEP * rows, 1), weighted

    def soften(t, slot):
        _, weighted = soft_part(slot, lane + off(t // HALVES), 0, window_blocks)
        wbuf[...] = weighted[:, :HD] / weighted[:, HD:]

    for k in (2, 3, 1):
        kv_quad(k).start()
    forward_kv(top_slot, 0, lambda copy: copy.start())

    own_codes.wait()

    @pl.when(has_down)
    def _():
        code_down(0).start()
    all_q.wait()
    for k in (1, 2, 3):
        q_quad(k).start()

    for edge, offset in ((0, reach * rows), (1, 0)):
        query = lax.broadcasted_iota(jnp.int32, (rows, rows), 0)
        key = lax.broadcasted_iota(jnp.int32, (rows, rows), 1) - offset
        gap = query - key
        bias[:, edge * rows:(edge + 1) * rows] = jnp.where((gap >= 0) & (gap < WINDOW), 0.0, -jnp.inf).astype(F32)
    for slot in range(slots):
        value = jnp.where(there(slot), 1.0, 0.0).astype(F32)
        ones[slot * QUAD:(slot + 1) * QUAD] = jnp.full((QUAD, rows, HD), value, F32).astype(BF16)

    def take_quad(k):
        kv_quad_in(k).wait_recv()
        forward_kv(top_slot, k, lambda copy: copy.start())

    def take_z(slot, k):
        @pl.when(there(slot))
        def _():
            z_kv(slot + 2, k).wait_recv()
        forward_kv(slot, k, lambda copy: copy.start())

    levels = range(top_slot - 2, -1, -2)
    take_quad(1)
    own_kv.wait()
    take_z(top_slot - 2, 0)
    take_z(top_slot - 2, 1)
    take_quad(2)
    take_quad(3)
    for slot in levels[1:]:
        take_z(slot, 0)
        take_z(slot, 1)
    take_z(top_slot - 2, 2)
    take_z(top_slot - 2, 3)

    for slot in levels[1:]:
        take_z(slot, 2)
        take_z(slot, 3)

    @pl.when(has_up)
    def _():
        code_up(0).start()
    send_y(z)

    run_events(-1)
    for slot in range(top_slot):
        @pl.when(jnp.logical_not(there(slot)))
        def _():
            first = win[top_slot * QUAD, 0:1, 0:HD].astype(F32)
            fill = jnp.concatenate([jnp.broadcast_to(first, (rows, HD)), jnp.zeros((rows, HD), F32)], axis=1)
            fill = fill.astype(BF16)
            for i in range(QUAD):
                win[slot * QUAD + i] = fill

    late_blocks = 2 * QUAD

    def take_y(slot):
        for k in range(QUAD):
            @pl.when(there(slot))
            def _():
                level = (top_slot - 1 - slot) // 2
                remote(block(slot, k), block(slot, k), ys.at[level, k], yr.at[level, k], me + dy).wait_recv()

    for slot in range(top_slot - 1, 1, -2):
        take_y(slot)
    own_q.wait()
    all_signs.wait()
    all_scales.wait()
    score(0, 0, late_blocks, window_blocks - late_blocks)
    near_top, near_sum = soft_part(0, lane, late_blocks, window_blocks - late_blocks)
    tops[...] = jnp.broadcast_to(near_top, tops.shape)
    sums[...] = near_sum
    take_y(1)
    score(0, 0, 0, late_blocks)
    far_top, far_sum = soft_part(0, lane, 0, late_blocks)
    both_top = jnp.maximum(tops[:, :1], far_top)
    weighted = sums[...] * jnp.exp2(tops[:, :1] - both_top) + far_sum * jnp.exp2(far_top - both_top)
    wbuf[...] = weighted[:, :HD] / weighted[:, HD:]

    def piece(r, source_lane, half):
        start = source_lane * width + half * half_width
        return rot.at[r, :, pl.ds(pl.multiple_of(start, half_width), half_width)]

    def rot_x(t):
        ref = piece(lane + off(t // 2), lane, t % 2)
        return remote(ref, ref, rx_s.at[t], rx_r.at[t], me + dx)

    def rot_c(t):
        ref = piece(lane + off(t // 2), lane, t % 2)
        return remote(ref, ref, rc_s.at[t], rc_r.at[t], me + dc)

    def rot_x_in(t):
        k = t // 2
        ref = piece(lane + dx + (k % 2) * dc - (k // 2) * dx, lane + dx, t % 2)
        return remote(ref, ref, rx_s.at[t], rx_r.at[t], me + dx)

    def rot_f(t):
        k = t // 2
        ref = piece(lane + dx + (k % 2) * dc - (k // 2) * dx, lane + dx, t % 2)
        return remote(ref, ref, rf_s.at[t], rf_r.at[t], me + dc)

    def rot_c_in(t):
        k = t // 2
        ref = piece(lane + dc - (k % 2) * dc + (k // 2) * dx, lane + dc, t % 2)
        return remote(ref, ref, rc_s.at[t], rc_r.at[t], me + dc)

    def rot_f_in(t):
        k = t // 2
        ref = piece(lane + dc + dx - (k % 2) * dc - (k // 2) * dx, lane + dc + dx, t % 2)
        return remote(ref, ref, rf_s.at[t], rf_r.at[t], me + dc)

    def rotate(t):
        k = t // HALVES
        half = t % HALVES
        signs = signs_buf[lane * HALVES + half].astype(F32)
        signed = wbuf[...].reshape(PER_STEP, rows, HD) * signs[:, None, :]
        signed = signed.reshape(PER_STEP * rows, HD)
        high = signed.astype(BF16)
        low = (signed - high.astype(F32)).astype(BF16)
        mixed = jnp.dot(high, had_ref[...], preferred_element_type=F32)
        mixed = mixed + jnp.dot(low, had_ref[...], preferred_element_type=F32)
        mixed = (mixed * (1.0 / math.sqrt(HD))).astype(BF16)
        start = lane * width + half * half_width
        for h in range(PER_STEP):
            rot[lane + off(k), :, pl.ds(pl.multiple_of(start + h * HD, HD), HD)] = mixed[h * rows:(h + 1) * rows]

    def publish(t):
        @pl.when(me < n)
        def _():
            rotate(t)

        @pl.when(t >= LAG)
        def _():
            rot_x_in(t - LAG).wait_recv()
            rot_f(t - LAG).start()

        run_events(t)
        rot_x(t).start()
        rot_c(t).start()

    def step(t, slot):
        score(jnp.minimum(t + 1, STEPS - 1), 1 - slot)
        soften(t, slot)
        publish(t)

    def attend(j, carry):
        k = j + 1
        remote(qbuf.at[k], qbuf.at[k], qs.at[k], qr.at[k], me + off(k)).wait_recv()
        step(2 * j + 1, 1)
        step(2 * j + 2, 0)
        return carry

    publish(jnp.int32(0))
    score(1, 1)
    lax.fori_loop(0, QUAD - 1, attend, 0)
    step(jnp.int32(STEPS - 1), 1)
    for t in range(STEPS - LAG, STEPS // 2):
        rot_x_in(t).wait_recv()
        rot_f(t).start()

    def gathered(t, carry):
        rot_c_in(t).wait_recv()
        return carry

    def gathered_far(t, carry):
        rot_f_in(t).wait_recv()
        return carry

    lax.fori_loop(0, STEPS, gathered, 0)
    lax.fori_loop(0, STEPS // 2, gathered_far, 0)
    chunk_heads = 8
    words = GROUP // 8

    def lanes_of(unit, source_lane):
        s = unit * QUAD + source_lane
        return pl.ds(pl.multiple_of(s * cols, cols), cols)

    def out_send(unit, k):
        target = out_ref.at[:, lanes_of(unit, lane)]
        return remote(stage.at[unit, lane + off(k)], target, os.at[unit, k], orr.at[unit, k], me + off(k))

    def out_recv(unit, k):
        target = out_ref.at[:, lanes_of(unit, lane + off(k))]
        return remote(target, target, os.at[unit, k], orr.at[unit, k], me + off(k))

    def out_own(unit):
        return pltpu.make_async_copy(stage.at[unit, lane], out_ref.at[:, lanes_of(unit, lane)], ol.at[unit])

    def project(unit, side):
        scale = scales[:, lanes_of(unit, lane)]
        acc = jnp.zeros((2 * rows, cols), F32)
        for chunk in range(HEADS // chunk_heads):
            parts = []
            for h in range(chunk * chunk_heads, (chunk + 1) * chunk_heads):
                word = cbuf[unit, h * words:(h + 1) * words, :] ^ jnp.int32(-2004318072)
                factor = jnp.broadcast_to(scale[h:h + 1, :], (words, cols))
                for k in range(8):
                    code = jnp.right_shift(jnp.left_shift(word, 28 - 4 * k), 28)
                    parts.append(code.astype(F32).astype(BF16) * factor)
            weight = jnp.concatenate(parts, axis=0)
            span = chunk_heads * HD
            lhs = rot[pl.ds(2 * side, 2), :, chunk * span:(chunk + 1) * span].reshape(2 * rows, span)
            acc = acc + jnp.dot(lhs, weight, preferred_element_type=F32)
        stage[unit, pl.ds(2 * side, 2)] = acc.astype(BF16).reshape(2, rows, cols)

        @pl.when(side == x)
        def _():
            out_send(unit, 1).start()
            out_own(unit).start()

        @pl.when(side != x)
        def _():
            out_send(unit, 2).start()
            out_send(unit, 3).start()

    def sweep(i, carry):
        first = i < 2 * early
        rest = i - 2 * early
        q = jnp.where(first, i % early, early + rest // 2)
        partner = jnp.where(first, i < early, rest % 2 == 0)
        plane = plane_at(q // 2)
        other = q % 2

        run_events(STEPS + i)

        @pl.when(i == early)
        def _():
            for t in range(max(STEPS - LAG, STEPS // 2), STEPS):
                rot_x_in(t).wait_recv()
                rot_f(t).start()
            lax.fori_loop(STEPS // 2, STEPS, gathered_far, 0)

        @pl.when(partner & (other == 1) & (plane != z))
        def _():
            wait_y(plane)

        project(plane * 2 + y + other * (1 - 2 * y), jnp.where(partner, 1 - x, x))
        return carry

    lax.fori_loop(0, 4 * planes, sweep, 0)

    for k in (1, 2, 3):
        kv_quad(k).wait_send()
        q_quad(k).wait_send()
    for slot in range(top_slot, -1, -2):
        for k in range(QUAD):
            forward_kv(slot, k, lambda copy: copy.wait_send())

    def drain_codes(k, carry):
        @pl.when((z - k >= 0) & has_up)
        def _():
            code_up(k).wait_send()

        @pl.when((z + k < planes) & has_down)
        def _():
            code_down(k).wait_send()
        each_y(k, y, lambda copy: copy.wait_send())
        return carry

    lax.fori_loop(0, planes, drain_codes, 0)

    @pl.when(has_up)
    def _():
        cross_up().wait_send()

    @pl.when(has_down)
    def _():
        cross_down().wait_send()

    def drain_rot(t, carry):
        rot_x(t).wait_send()
        rot_c(t).wait_send()
        rot_f(t).wait_send()
        return carry

    lax.fori_loop(0, STEPS, drain_rot, 0)

    def drain_out(unit, carry):
        out_own(unit).wait()
        for k in (1, 2, 3):
            out_send(unit, k).wait_send()
            out_recv(unit, k).wait_recv()
        return carry

    lax.fori_loop(0, 2 * planes, drain_out, 0)


def on_device(queries, keys_values, head_signs, out_codes, out_scales):
    n = lax.axis_size("seq")
    rows = queries.shape[0]
    reach = (WINDOW + rows - 2) // rows
    span = -(-reach // QUAD)
    slots = span + 1
    assert slots % 2 == 1
    planes = n // (2 * QUAD)
    word_rows, cols = out_codes.shape
    vmem = pl.BlockSpec(memory_space=pltpu.VMEM)
    hbm = pl.BlockSpec(memory_space=pltpu.HBM)
    in_hbm = functools.partial(pltpu.with_memory_space_constraint, memory_space=pltpu.HBM)
    dma = pltpu.SemaphoreType.DMA
    return pl.pallas_call(
        functools.partial(kernel, n, reach, slots),
        out_shape=pltpu.VMEM((rows, n * cols), BF16),
        in_specs=[hbm, hbm, hbm, vmem, hbm, hbm],
        out_specs=pl.BlockSpec(memory_space=pl.ANY),
        scratch_shapes=[
            pltpu.VMEM((slots * QUAD, rows, 2 * HD), BF16),
            pltpu.VMEM((slots * QUAD, rows, HD), BF16),
            pltpu.VMEM((QUAD, rows, LANE_HEADS * HD), BF16),
            pltpu.VMEM((2 * planes, word_rows, cols), jnp.int32),
            pltpu.VMEM((QUAD, rows, HEADS * HD), BF16),
            pltpu.VMEM((rows, 2 * rows), F32),
            pltpu.VMEM((2, PER_STEP * rows, (reach + 1) * rows), F32),
            pltpu.VMEM((PER_STEP * rows, HD), F32),
            pltpu.VMEM((PER_STEP * rows, HD), F32),
            pltpu.VMEM((PER_STEP * rows, 2 * HD), F32),
            pltpu.VMEM((2 * planes, QUAD, rows, cols), BF16),
            pltpu.VMEM((rows, HEADS * HD), BF16),
            pltpu.VMEM((STEPS, PER_STEP, HD), jnp.int32),
            pltpu.VMEM((HEADS, n * cols), BF16),
            pltpu.VMEM((rows, 2, KV * HD), BF16),
            pltpu.VMEM((KV, rows, 2 * HD), BF16),
            dma((7,)),
            dma((QUAD,)), dma((QUAD,)),
            dma((QUAD,)), dma((QUAD,)),
            dma((slots // 2, QUAD)), dma((slots // 2, QUAD)),
            dma((slots // 2, QUAD)), dma((slots // 2, QUAD)),
            dma((planes + 1,)), dma((planes + 1,)),
            dma((planes + 1,)), dma((planes + 1,)),
            dma((planes,)), dma((planes,)),
            dma((2,)), dma((2,)),
            dma((STEPS,)), dma((STEPS,)),
            dma((STEPS,)), dma((STEPS,)),
            dma((STEPS,)), dma((STEPS,)),
            dma((2 * planes, QUAD)), dma((2 * planes, QUAD)),
            dma((2 * planes,)),
        ],
        compiler_params=pltpu.CompilerParams(
            collective_id=0, has_side_effects=True, vmem_limit_bytes=52 * 1000 * 1000
        ),
    )(
        in_hbm(queries),
        in_hbm(keys_values),
        in_hbm(head_signs.reshape(STEPS, PER_STEP, HD)),
        reordered_hadamard(),
        in_hbm(out_codes),
        in_hbm(out_scales),
    )


def solution(mesh):
    return jax.shard_map(
        on_device,
        mesh=mesh,
        in_specs=(
            P(("groups", "seq"), None),
            P(("groups", "seq"), None, None),
            P(),
            P(None, "seq"),
            P(),
        ),
        out_specs=P(("groups", "seq"), None),
        check_vma=False,
    )
```

```python
import functools
import math

import jax
import jax.numpy as jnp
from jax import lax
from jax.experimental import pallas as pl
from jax.experimental.pallas import tpu as pltpu
from jax.sharding import PartitionSpec as P

HEADS = 32
KV = 4
HD = 128
GROUP = 128
WINDOW = 2048
QUAD = 4
LANE_HEADS = HEADS // QUAD
HALVES = 2
PER_STEP = LANE_HEADS // HALVES
STEPS = QUAD * HALVES
LAG = 5
LOG2E = 1.4426950408889634
MESH = pl.DeviceIdType.MESH
BF16 = jnp.bfloat16
F32 = jnp.float32


def reordered_hadamard():
    column = jnp.arange(HD, dtype=jnp.int32)
    source = (column % 16) * 8 + column // 16
    common = jnp.bitwise_and(jnp.arange(HD, dtype=jnp.int32)[:, None], source[None, :])
    ones = jnp.zeros((HD, HD), jnp.int32)
    for bit in range(HD.bit_length()):
        ones = ones + jnp.bitwise_and(jnp.right_shift(common, bit), 1)
    return jnp.where(ones % 2 == 0, 1.0, -1.0).astype(BF16)


def kernel(
    n, reach, slots,
    q_ref, kv_ref, sign_ref, had_ref, codes_ref, scales_ref, out_ref,
    win, ones, qbuf, cbuf, rot, bias, sbuf, wbuf, tops, sums, stage,
    q_all, signs_buf, scales, kv_raw, kv_heads, local_sem,
    kq_s, kq_r, qs, qr, zs, zr, ys, yr, up_s, up_r, dn_s, dn_r, cy_s, cy_r, cross_s, cross_r,
    rx_s, rx_r, rc_s, rc_r, rf_s, rf_r, os, orr, ol,
):
    rows = q_ref.shape[0]
    cols = codes_ref.shape[1]
    planes = n // (2 * QUAD)
    width = LANE_HEADS * HD
    half_width = PER_STEP * HD
    top_slot = slots - 1
    me = lax.axis_index("seq")
    z = me // (2 * QUAD)
    y = (me // QUAD) % 2
    lane = me % QUAD
    quad = me // QUAD
    core, x = lane % 2, lane // 2
    dc, dx, dy = 1 - 2 * core, 2 - 4 * x, QUAD - 2 * QUAD * y
    up, down = me + 2 * QUAD, me - 2 * QUAD
    has_up, has_down = z + 1 < planes, z >= 1

    def off(k):
        return (k % 2) * dc + (k // 2) * dx

    def remote(src, dst, send, recv, target):
        return pltpu.make_async_remote_copy(
            src_ref=src, dst_ref=dst, send_sem=send, recv_sem=recv,
            device_id={"seq": target}, device_id_type=MESH,
        )

    window_blocks = reach + 1
    keys = window_blocks * rows
    raw_kv = pltpu.make_async_copy(kv_ref, kv_raw, local_sem.at[6])
    own_kv = pltpu.make_async_copy(
        kv_heads.at[lane], win.at[top_slot * QUAD + lane, :, pl.ds(0, 2 * HD)], local_sem.at[0])
    own_lanes = pl.ds(pl.multiple_of(lane * width, width), width)
    all_q = pltpu.make_async_copy(q_ref, q_all, local_sem.at[5])
    own_q = pltpu.make_async_copy(q_ref.at[:, own_lanes], qbuf.at[0], local_sem.at[1])
    own_codes = pltpu.make_async_copy(codes_ref, cbuf.at[quad], local_sem.at[2])
    all_signs = pltpu.make_async_copy(sign_ref, signs_buf, local_sem.at[3])
    all_scales = pltpu.make_async_copy(scales_ref, scales, local_sem.at[4])
    for copy in (raw_kv, all_q, own_codes, own_q, all_signs, all_scales):
        copy.start()

    barrier = pltpu.get_barrier_semaphore()

    def greet(target):
        pl.semaphore_signal(barrier, inc=1, device_id={"seq": target}, device_id_type=MESH)

    for k in (2, 3, 1):
        greet(me + off(k))
    greet(me + dy)

    @pl.when(has_up)
    def _():
        greet(up)

    @pl.when(has_down)
    def _():
        greet(down)

    raw_kv.wait()
    pairs = kv_raw[...].reshape(2 * rows, KV * HD)
    to = lax.broadcasted_iota(jnp.int32, (rows, 2 * rows), 0)
    source_row = lax.broadcasted_iota(jnp.int32, (rows, 2 * rows), 1)
    for which in range(2):
        pick = jnp.where(source_row == 2 * to + which, 1.0, 0.0).astype(BF16)
        picked = jnp.dot(pick, pairs, preferred_element_type=F32).astype(BF16)
        for g in range(KV):
            kv_heads[g, :, which * HD:(which + 1) * HD] = picked[:, g * HD:(g + 1) * HD]
    pl.semaphore_wait(barrier, QUAD + has_up.astype(jnp.int32) + has_down.astype(jnp.int32))

    own_kv.start()
    def part_lanes(k):
        return pl.ds((k % 2) * HD, HD)

    def block(slot, k):
        return win.at[slot * QUAD + lane + off(k // 2), :, part_lanes(k)]

    def kv_quad(k):
        return remote(kv_heads.at[lane + off(k // 2), :, part_lanes(k)],
                      win.at[top_slot * QUAD + lane, :, part_lanes(k)],
                      kq_s.at[k], kq_r.at[k], me + off(k // 2))

    def kv_quad_in(k):
        return remote(block(top_slot, k), block(top_slot, k), kq_s.at[k], kq_r.at[k], me + off(k // 2))

    def source(slot, k):
        return kv_heads.at[lane, :, part_lanes(k)] if slot == top_slot and k < 2 else block(slot, k)

    def z_kv(slot, k):
        return remote(source(slot, k), block(slot - 2, k),
                      zs.at[(top_slot - slot) // 2, k], zr.at[(top_slot - slot) // 2, k], up)

    def y_kv(slot, target, k):
        level = (top_slot - 1 - target) // 2
        return remote(source(slot, k), block(target, k), ys.at[level, k], yr.at[level, k], me + dy)

    def there(slot):
        return quad - top_slot + slot >= 0

    def forward_kv(slot, k, act):
        if slot >= 2:
            @pl.when(there(slot) & has_up)
            def _():
                act(z_kv(slot, k))
        if slot >= 1:
            @pl.when(there(slot) & (y == 0))
            def _():
                act(y_kv(slot, slot - 1, k))
        if slot + 1 < top_slot:
            @pl.when(there(slot) & (y == 1))
            def _():
                act(y_kv(slot, slot + 1, k))

    def q_quad(k):
        lanes = pl.ds(pl.multiple_of((lane + off(k)) * width, width), width)
        return remote(q_all.at[:, lanes], qbuf.at[k], qs.at[k], qr.at[k], me + off(k))

    def code_up(k):
        unit = cbuf.at[quad - 2 * k]
        return remote(unit, unit, up_s.at[k + 1], up_r.at[k + 1], up)

    def code_up_in(k):
        unit = cbuf.at[quad - 2 * k]
        return remote(unit, unit, up_s.at[k], up_r.at[k], up)

    def code_down(k):
        unit = cbuf.at[quad + 2 * k]
        return remote(unit, unit, dn_s.at[k + 1], dn_r.at[k + 1], down)

    def code_down_in(k):
        unit = cbuf.at[quad + 2 * k]
        return remote(unit, unit, dn_s.at[k], dn_r.at[k], down)

    half_words = cbuf.shape[1] // 2

    def far(plane):
        return ((plane == 0) | (plane == planes - 1)) & (plane != z)

    def each_y(plane, column, act):
        def copy(unit):
            return remote(unit, unit, cy_s.at[plane], cy_r.at[plane], me + dy)

        @pl.when(far(plane))
        def _():
            act(copy(cbuf.at[plane * 2 + column, pl.ds(0, half_words)]))

        @pl.when(jnp.logical_not(far(plane)))
        def _():
            act(copy(cbuf.at[plane * 2 + column]))

    def send_y(plane):
        each_y(plane, y, lambda copy: copy.start())

    def wait_y(plane):
        each_y(plane, 1 - y, lambda copy: copy.wait_recv())

    def cross_up():
        unit = cbuf.at[1 - y, pl.ds(half_words, half_words)]
        return remote(unit, unit, cross_s.at[0], cross_r.at[0], up)

    def cross_down():
        unit = cbuf.at[(planes - 1) * 2 + 1 - y, pl.ds(half_words, half_words)]
        return remote(unit, unit, cross_s.at[1], cross_r.at[1], down)

    near = jnp.minimum(z, planes - 1 - z)
    toward = jnp.where(z <= planes - 1 - z, 1, -1)

    def plane_at(p):
        both = z + ((p + 1) // 2) * (2 * (p % 2) - 1)
        return jnp.where(p <= 2 * near, both, z + toward * (p - near))

    early = planes + 1

    def relay(p):
        plane = plane_at(p)

        @pl.when(plane < z)
        def _():
            code_up_in(z - plane).wait_recv()

            @pl.when(has_up)
            def _():
                code_up(z - plane).start()
            send_y(plane)

        @pl.when(plane > z)
        def _():
            code_down_in(plane - z).wait_recv()

            @pl.when(has_down)
            def _():
                code_down(plane - z).start()
            send_y(plane)

    def own_y():
        wait_y(z)

        @pl.when((z == 0) & has_up)
        def _():
            cross_up().start()

        @pl.when((z == planes - 1) & has_down)
        def _():
            cross_down().start()

    def relay_cross_up():
        @pl.when(has_down)
        def _():
            cross_up().wait_recv()

            @pl.when(has_up)
            def _():
                cross_up().start()

    def relay_cross_down():
        @pl.when(has_up)
        def _():
            cross_down().wait_recv()

            @pl.when(has_down)
            def _():
                cross_down().start()

    begin = jnp.where(z == 0, 80, jnp.where(z == 1, 138, 165))
    after = jnp.where(z == 0, 295, jnp.where(z == 1, 318, 335))
    stall = 55

    def item_of(q):
        return STEPS + jnp.where(q < early, q, 2 * early + 2 * (q - early))

    events = []

    def expect(action, arrival, deadline, prologue=None):
        step_at = jnp.clip((arrival - begin - 10) // 20, 0, STEPS - 1)
        wait = arrival - after
        later = early + jnp.maximum(wait - 9 * early - stall, 0) // 9
        item_at = STEPS + jnp.where(wait < 9 * early, wait // 9, later)
        at = jnp.minimum(jnp.where(arrival < after, step_at, item_at), deadline)
        if prologue is not None:
            at = jnp.where(prologue, -1, at)
        events.append((action, arrival, at))

    for p in range(1, planes):
        d = plane_at(p) - z
        arrival = jnp.where(d > 0, 130 * d, jnp.where(z == 1, 71, 130) - 117 * d)
        expect(functools.partial(relay, p), arrival, item_of(2 * p - 1), (d == 1) & has_down)
    expect(own_y, jnp.where(z == 0, 185, jnp.where(z == 1, 255, 290)), item_of(1))
    bottom = jnp.where(z == near, 2 * z, planes - 1)
    top_at = jnp.where(planes - 1 - z == near, 2 * near - 1, planes - 1)
    expect(relay_cross_up, jnp.where(z == 1, 275, 170 + 130 * z), item_of(2 * bottom + 1))
    expect(relay_cross_down, 290 + 71 * (planes - 1 - z), item_of(2 * jnp.maximum(top_at, 0) + 1))
    timed = []
    for action, arrival, _ in events:
        at = None
        for _, other_arrival, other_at in events:
            later = jnp.where(other_arrival >= arrival, other_at, STEPS + 4 * planes)
            at = later if at is None else jnp.minimum(at, later)
        timed.append((action, at))

    def run_events(now):
        for action, at in timed:
            pl.when(at == now)(action)

    def score(t, slot, first=0, count=None):
        count = window_blocks if count is None else count
        k = t // HALVES
        half = t % HALVES
        lanes = pl.ds(pl.multiple_of(half * half_width, half_width), half_width)
        q = qbuf[k, :, lanes]
        q = jnp.concatenate([q[:, h * HD:(h + 1) * HD] for h in range(PER_STEP)], axis=0)
        scaled = q.astype(F32) * (LOG2E / math.sqrt(HD))
        high = scaled.astype(BF16)
        low = (scaled - high.astype(F32)).astype(BF16)
        q = jnp.concatenate([high, low], axis=1)
        k_rows = win[pl.ds(lane + off(k) + first, count), :, 0:HD].reshape(count * rows, HD)
        k_rows = jnp.concatenate([k_rows, k_rows], axis=1)
        part = lax.dot_general(q, k_rows, (((1,), (1,)), ((), ())), preferred_element_type=F32)
        sbuf[slot, :, first * rows:(first + count) * rows] = part

    def soft_part(slot, r, first, count):
        scores = sbuf[slot, :, first * rows:(first + count) * rows].reshape(PER_STEP, rows, count * rows)
        head, tail = rows if first == 0 else 0, rows if first + count == window_blocks else 0
        parts = [scores[:, :, head:count * rows - tail]]
        if head:
            parts.insert(0, scores[:, :, :head] + bias[:, :rows][None])
        if tail:
            parts.append(scores[:, :, count * rows - tail:] + bias[:, rows:][None])
        scores = jnp.concatenate(parts, axis=2)
        top = jnp.max(scores, axis=-1, keepdims=True)
        weights = jnp.exp2(scores - top).astype(BF16)
        v_rows = win[pl.ds(r + first, count), :, HD:2 * HD].reshape(count * rows, HD)
        v_rows = jnp.concatenate([v_rows, ones[pl.ds(r + first, count)].reshape(count * rows, HD)], axis=1)
        weighted = jnp.dot(weights.reshape(PER_STEP * rows, count * rows), v_rows, preferred_element_type=F32)
        return top.reshape(PER_STEP * rows, 1), weighted

    def soften(t, slot):
        _, weighted = soft_part(slot, lane + off(t // HALVES), 0, window_blocks)
        wbuf[...] = weighted[:, :HD] / weighted[:, HD:]

    for k in (4, 6, 2, 5, 7, 3):
        kv_quad(k).start()
    for k in (0, 1):
        forward_kv(top_slot, k, lambda copy: copy.start())

    own_codes.wait()

    @pl.when(has_down)
    def _():
        code_down(0).start()
    all_q.wait()
    for k in (1, 2, 3):
        q_quad(k).start()

    for edge, offset in ((0, reach * rows), (1, 0)):
        query = lax.broadcasted_iota(jnp.int32, (rows, rows), 0)
        key = lax.broadcasted_iota(jnp.int32, (rows, rows), 1) - offset
        gap = query - key
        bias[:, edge * rows:(edge + 1) * rows] = jnp.where((gap >= 0) & (gap < WINDOW), 0.0, -jnp.inf).astype(F32)
    for slot in range(slots):
        value = jnp.where(there(slot), 1.0, 0.0).astype(F32)
        ones[slot * QUAD:(slot + 1) * QUAD] = jnp.full((QUAD, rows, HD), value, F32).astype(BF16)

    def take_quad(k):
        kv_quad_in(k).wait_recv()
        forward_kv(top_slot, k, lambda copy: copy.start())

    def take_z(slot, k):
        @pl.when(there(slot))
        def _():
            z_kv(slot + 2, k).wait_recv()
        forward_kv(slot, k, lambda copy: copy.start())

    levels = range(top_slot - 2, -1, -2)
    for k in (2, 3):
        take_quad(k)
    own_kv.wait()
    for k in (0, 1, 2, 3):
        take_z(top_slot - 2, k)
    for k in (4, 6, 5, 7):
        take_quad(k)
    for slot in levels[1:]:
        for k in (0, 1, 2, 3):
            take_z(slot, k)
    for k in (4, 6, 5, 7):
        take_z(top_slot - 2, k)

    for slot in levels[1:]:
        for k in (4, 6, 5, 7):
            take_z(slot, k)

    @pl.when(has_up)
    def _():
        code_up(0).start()

    def open_y():
        send_y(z)
        run_events(-1)

    open_y()
    for slot in range(top_slot):
        @pl.when(jnp.logical_not(there(slot)))
        def _():
            first = win[top_slot * QUAD, 0:1, 0:HD].astype(F32)
            fill = jnp.concatenate([jnp.broadcast_to(first, (rows, HD)), jnp.zeros((rows, HD), F32)], axis=1)
            fill = fill.astype(BF16)
            for i in range(QUAD):
                win[slot * QUAD + i] = fill

    late_blocks = 2 * QUAD

    def take_y(slot, pieces):
        for k in pieces:
            @pl.when(there(slot))
            def _():
                level = (top_slot - 1 - slot) // 2
                remote(block(slot, k), block(slot, k), ys.at[level, k], yr.at[level, k], me + dy).wait_recv()

    for slot in range(top_slot - 1, 1, -2):
        take_y(slot, range(2 * QUAD))
    own_q.wait()
    all_signs.wait()
    all_scales.wait()
    score(0, 0, late_blocks, window_blocks - late_blocks)
    near_top, near_sum = soft_part(0, lane, late_blocks, window_blocks - late_blocks)
    tops[...] = jnp.broadcast_to(near_top, tops.shape)
    sums[...] = near_sum
    take_y(1, range(0, 2 * QUAD, 2))
    score(0, 0, 0, late_blocks)
    take_y(1, range(1, 2 * QUAD, 2))
    far_top, far_sum = soft_part(0, lane, 0, late_blocks)
    both_top = jnp.maximum(tops[:, :1], far_top)
    weighted = sums[...] * jnp.exp2(tops[:, :1] - both_top) + far_sum * jnp.exp2(far_top - both_top)
    wbuf[...] = weighted[:, :HD] / weighted[:, HD:]

    def piece(r, source_lane, half):
        start = source_lane * width + half * half_width
        return rot.at[r, :, pl.ds(pl.multiple_of(start, half_width), half_width)]

    def rot_x(t):
        ref = piece(lane + off(t // 2), lane, t % 2)
        return remote(ref, ref, rx_s.at[t], rx_r.at[t], me + dx)

    def rot_c(t):
        ref = piece(lane + off(t // 2), lane, t % 2)
        return remote(ref, ref, rc_s.at[t], rc_r.at[t], me + dc)

    def rot_x_in(t):
        k = t // 2
        ref = piece(lane + dx + (k % 2) * dc - (k // 2) * dx, lane + dx, t % 2)
        return remote(ref, ref, rx_s.at[t], rx_r.at[t], me + dx)

    def rot_f(t):
        k = t // 2
        ref = piece(lane + dx + (k % 2) * dc - (k // 2) * dx, lane + dx, t % 2)
        return remote(ref, ref, rf_s.at[t], rf_r.at[t], me + dc)

    def rot_c_in(t):
        k = t // 2
        ref = piece(lane + dc - (k % 2) * dc + (k // 2) * dx, lane + dc, t % 2)
        return remote(ref, ref, rc_s.at[t], rc_r.at[t], me + dc)

    def rot_f_in(t):
        k = t // 2
        ref = piece(lane + dc + dx - (k % 2) * dc - (k // 2) * dx, lane + dc + dx, t % 2)
        return remote(ref, ref, rf_s.at[t], rf_r.at[t], me + dc)

    def rotate(t):
        k = t // HALVES
        half = t % HALVES
        signs = signs_buf[lane * HALVES + half].astype(F32)
        signed = wbuf[...].reshape(PER_STEP, rows, HD) * signs[:, None, :]
        signed = signed.reshape(PER_STEP * rows, HD)
        high = signed.astype(BF16)
        low = (signed - high.astype(F32)).astype(BF16)
        mixed = jnp.dot(high, had_ref[...], preferred_element_type=F32)
        mixed = mixed + jnp.dot(low, had_ref[...], preferred_element_type=F32)
        mixed = (mixed * (1.0 / math.sqrt(HD))).astype(BF16)
        start = lane * width + half * half_width
        for h in range(PER_STEP):
            rot[lane + off(k), :, pl.ds(pl.multiple_of(start + h * HD, HD), HD)] = mixed[h * rows:(h + 1) * rows]

    def publish(t):
        @pl.when(me < n)
        def _():
            rotate(t)

        @pl.when(t >= LAG)
        def _():
            rot_x_in(t - LAG).wait_recv()
            rot_f(t - LAG).start()

        run_events(t)
        rot_x(t).start()
        rot_c(t).start()

    def step(t, slot):
        score(jnp.minimum(t + 1, STEPS - 1), 1 - slot)
        soften(t, slot)
        publish(t)

    def attend(j, carry):
        k = j + 1
        remote(qbuf.at[k], qbuf.at[k], qs.at[k], qr.at[k], me + off(k)).wait_recv()
        step(2 * j + 1, 1)
        step(2 * j + 2, 0)
        return carry

    publish(jnp.int32(0))
    score(1, 1)
    lax.fori_loop(0, QUAD - 1, attend, 0)
    step(jnp.int32(STEPS - 1), 1)
    for t in range(STEPS - LAG, STEPS // 2):
        rot_x_in(t).wait_recv()
        rot_f(t).start()

    def gathered(t, carry):
        rot_c_in(t).wait_recv()
        return carry

    def gathered_far(t, carry):
        rot_f_in(t).wait_recv()
        return carry

    lax.fori_loop(0, STEPS, gathered, 0)
    lax.fori_loop(0, STEPS // 2, gathered_far, 0)
    chunk_heads = 8
    words = GROUP // 8

    def lanes_of(unit, source_lane):
        s = unit * QUAD + source_lane
        return pl.ds(pl.multiple_of(s * cols, cols), cols)

    def out_send(unit, k):
        target = out_ref.at[:, lanes_of(unit, lane)]
        return remote(stage.at[unit, lane + off(k)], target, os.at[unit, k], orr.at[unit, k], me + off(k))

    def out_recv(unit, k):
        target = out_ref.at[:, lanes_of(unit, lane + off(k))]
        return remote(target, target, os.at[unit, k], orr.at[unit, k], me + off(k))

    def out_own(unit):
        return pltpu.make_async_copy(stage.at[unit, lane], out_ref.at[:, lanes_of(unit, lane)], ol.at[unit])

    def project(unit, side):
        scale = scales[:, lanes_of(unit, lane)]
        acc = jnp.zeros((2 * rows, cols), F32)
        for chunk in range(HEADS // chunk_heads):
            parts = []
            for h in range(chunk * chunk_heads, (chunk + 1) * chunk_heads):
                word = cbuf[unit, h * words:(h + 1) * words, :] ^ jnp.int32(-2004318072)
                factor = jnp.broadcast_to(scale[h:h + 1, :], (words, cols))
                for k in range(8):
                    code = jnp.right_shift(jnp.left_shift(word, 28 - 4 * k), 28)
                    parts.append(code.astype(F32).astype(BF16) * factor)
            weight = jnp.concatenate(parts, axis=0)
            span = chunk_heads * HD
            lhs = rot[pl.ds(2 * side, 2), :, chunk * span:(chunk + 1) * span].reshape(2 * rows, span)
            acc = acc + jnp.dot(lhs, weight, preferred_element_type=F32)
        stage[unit, pl.ds(2 * side, 2)] = acc.astype(BF16).reshape(2, rows, cols)

        @pl.when(side == x)
        def _():
            out_send(unit, 1).start()
            out_own(unit).start()

        @pl.when(side != x)
        def _():
            out_send(unit, 2).start()
            out_send(unit, 3).start()

    def sweep(i, carry):
        first = i < 2 * early
        rest = i - 2 * early
        q = jnp.where(first, i % early, early + rest // 2)
        partner = jnp.where(first, i < early, rest % 2 == 0)
        plane = plane_at(q // 2)
        other = q % 2

        run_events(STEPS + i)

        @pl.when(i == early)
        def _():
            for t in range(max(STEPS - LAG, STEPS // 2), STEPS):
                rot_x_in(t).wait_recv()
                rot_f(t).start()
            lax.fori_loop(STEPS // 2, STEPS, gathered_far, 0)

        @pl.when(partner & (other == 1) & (plane != z))
        def _():
            wait_y(plane)

        project(plane * 2 + y + other * (1 - 2 * y), jnp.where(partner, 1 - x, x))
        return carry

    lax.fori_loop(0, 4 * planes, sweep, 0)

    for k in (1, 2, 3):
        q_quad(k).wait_send()
    for k in range(2, 2 * QUAD):
        kv_quad(k).wait_send()
    for slot in range(top_slot, -1, -2):
        for k in range(2 * QUAD):
            forward_kv(slot, k, lambda copy: copy.wait_send())

    def drain_codes(k, carry):
        @pl.when((z - k >= 0) & has_up)
        def _():
            code_up(k).wait_send()

        @pl.when((z + k < planes) & has_down)
        def _():
            code_down(k).wait_send()
        each_y(k, y, lambda copy: copy.wait_send())
        return carry

    lax.fori_loop(0, planes, drain_codes, 0)

    @pl.when(has_up)
    def _():
        cross_up().wait_send()

    @pl.when(has_down)
    def _():
        cross_down().wait_send()

    def drain_rot(t, carry):
        rot_x(t).wait_send()
        rot_c(t).wait_send()
        rot_f(t).wait_send()
        return carry

    lax.fori_loop(0, STEPS, drain_rot, 0)

    def drain_sent(unit, carry):
        out_own(unit).wait()
        for k in (1, 2, 3):
            out_send(unit, k).wait_send()
        return carry

    lax.fori_loop(0, 2 * planes, drain_sent, 0)

    def drain_out(q, carry):
        unit = plane_at(q // 2) * 2 + y + (q % 2) * (1 - 2 * y)
        for k in (1, 2, 3):
            out_recv(unit, k).wait_recv()
        return carry

    lax.fori_loop(0, 2 * planes, drain_out, 0)


def on_device(queries, keys_values, head_signs, out_codes, out_scales):
    n = lax.axis_size("seq")
    rows = queries.shape[0]
    reach = (WINDOW + rows - 2) // rows
    span = -(-reach // QUAD)
    slots = span + 1
    assert slots % 2 == 1
    planes = n // (2 * QUAD)
    word_rows, cols = out_codes.shape
    vmem = pl.BlockSpec(memory_space=pltpu.VMEM)
    hbm = pl.BlockSpec(memory_space=pltpu.HBM)
    in_hbm = functools.partial(pltpu.with_memory_space_constraint, memory_space=pltpu.HBM)
    dma = pltpu.SemaphoreType.DMA
    return pl.pallas_call(
        functools.partial(kernel, n, reach, slots),
        out_shape=pltpu.VMEM((rows, n * cols), BF16),
        in_specs=[hbm, hbm, hbm, vmem, hbm, hbm],
        out_specs=pl.BlockSpec(memory_space=pl.ANY),
        scratch_shapes=[
            pltpu.VMEM((slots * QUAD, rows, 2 * HD), BF16),
            pltpu.VMEM((slots * QUAD, rows, HD), BF16),
            pltpu.VMEM((QUAD, rows, LANE_HEADS * HD), BF16),
            pltpu.VMEM((2 * planes, word_rows, cols), jnp.int32),
            pltpu.VMEM((QUAD, rows, HEADS * HD), BF16),
            pltpu.VMEM((rows, 2 * rows), F32),
            pltpu.VMEM((2, PER_STEP * rows, (reach + 1) * rows), F32),
            pltpu.VMEM((PER_STEP * rows, HD), F32),
            pltpu.VMEM((PER_STEP * rows, HD), F32),
            pltpu.VMEM((PER_STEP * rows, 2 * HD), F32),
            pltpu.VMEM((2 * planes, QUAD, rows, cols), BF16),
            pltpu.VMEM((rows, HEADS * HD), BF16),
            pltpu.VMEM((STEPS, PER_STEP, HD), jnp.int32),
            pltpu.VMEM((HEADS, n * cols), BF16),
            pltpu.VMEM((rows, 2, KV * HD), BF16),
            pltpu.VMEM((KV, rows, 2 * HD), BF16),
            dma((7,)),
            dma((2 * QUAD,)), dma((2 * QUAD,)),
            dma((QUAD,)), dma((QUAD,)),
            dma((slots // 2, 2 * QUAD)), dma((slots // 2, 2 * QUAD)),
            dma((slots // 2, 2 * QUAD)), dma((slots // 2, 2 * QUAD)),
            dma((planes + 1,)), dma((planes + 1,)),
            dma((planes + 1,)), dma((planes + 1,)),
            dma((planes,)), dma((planes,)),
            dma((2,)), dma((2,)),
            dma((STEPS,)), dma((STEPS,)),
            dma((STEPS,)), dma((STEPS,)),
            dma((STEPS,)), dma((STEPS,)),
            dma((2 * planes, QUAD)), dma((2 * planes, QUAD)),
            dma((2 * planes,)),
        ],
        compiler_params=pltpu.CompilerParams(
            collective_id=0, has_side_effects=True, vmem_limit_bytes=52 * 1000 * 1000
        ),
    )(
        in_hbm(queries),
        in_hbm(keys_values),
        in_hbm(head_signs.reshape(STEPS, PER_STEP, HD)),
        reordered_hadamard(),
        in_hbm(out_codes),
        in_hbm(out_scales),
    )


def solution(mesh):
    return jax.shard_map(
        on_device,
        mesh=mesh,
        in_specs=(
            P(("groups", "seq"), None),
            P(("groups", "seq"), None, None),
            P(),
            P(None, "seq"),
            P(),
        ),
        out_specs=P(("groups", "seq"), None),
        check_vma=False,
    )
```

```python
import functools
import math

import jax
import jax.numpy as jnp
from jax import lax
from jax.experimental import pallas as pl
from jax.experimental.pallas import tpu as pltpu
from jax.sharding import PartitionSpec as P

HEADS = 32
KV = 4
HD = 128
GROUP = 128
WINDOW = 2048
QUAD = 4
LANE_HEADS = HEADS // QUAD
HALVES = 2
PER_STEP = LANE_HEADS // HALVES
STEPS = QUAD * HALVES
LAG = 5
LOG2E = 1.4426950408889634
MESH = pl.DeviceIdType.MESH
BF16 = jnp.bfloat16
F32 = jnp.float32


def reordered_hadamard():
    column = jnp.arange(HD, dtype=jnp.int32)
    source = (column % 16) * 8 + column // 16
    common = jnp.bitwise_and(jnp.arange(HD, dtype=jnp.int32)[:, None], source[None, :])
    ones = jnp.zeros((HD, HD), jnp.int32)
    for bit in range(HD.bit_length()):
        ones = ones + jnp.bitwise_and(jnp.right_shift(common, bit), 1)
    return jnp.where(ones % 2 == 0, 1.0, -1.0).astype(BF16)


def kernel(
    n, reach, slots,
    q_ref, kv_ref, sign_ref, had_ref, codes_ref, scales_ref, out_ref,
    win, ones, qbuf, cbuf, rot, bias, sbuf, wbuf, tops, sums, stage,
    q_all, signs_buf, scales, kv_raw, kv_heads, local_sem,
    kq_s, kq_r, qs, qr, zs, zr, ys, yr, up_s, up_r, dn_s, dn_r, cy_s, cy_r, cross_s, cross_r,
    rx_s, rx_r, rc_s, rc_r, rf_s, rf_r, os, orr, ol,
):
    rows = q_ref.shape[0]
    cols = codes_ref.shape[1]
    planes = n // (2 * QUAD)
    width = LANE_HEADS * HD
    half_width = PER_STEP * HD
    top_slot = slots - 1
    me = lax.axis_index("seq")
    z = me // (2 * QUAD)
    y = (me // QUAD) % 2
    lane = me % QUAD
    quad = me // QUAD
    core, x = lane % 2, lane // 2
    dc, dx, dy = 1 - 2 * core, 2 - 4 * x, QUAD - 2 * QUAD * y
    up, down = me + 2 * QUAD, me - 2 * QUAD
    has_up, has_down = z + 1 < planes, z >= 1

    def off(k):
        return (k % 2) * dc + (k // 2) * dx

    def remote(src, dst, send, recv, target):
        return pltpu.make_async_remote_copy(
            src_ref=src, dst_ref=dst, send_sem=send, recv_sem=recv,
            device_id={"seq": target}, device_id_type=MESH,
        )

    window_blocks = reach + 1
    keys = window_blocks * rows
    raw_kv = pltpu.make_async_copy(kv_ref, kv_raw, local_sem.at[6])
    own_kv = pltpu.make_async_copy(
        kv_heads.at[lane], win.at[top_slot * QUAD + lane, :, pl.ds(0, 2 * HD)], local_sem.at[0])
    own_lanes = pl.ds(pl.multiple_of(lane * width, width), width)
    all_q = pltpu.make_async_copy(q_ref, q_all, local_sem.at[5])
    own_q = pltpu.make_async_copy(q_ref.at[:, own_lanes], qbuf.at[0], local_sem.at[1])
    own_codes = pltpu.make_async_copy(codes_ref, cbuf.at[quad], local_sem.at[2])
    all_signs = pltpu.make_async_copy(sign_ref, signs_buf, local_sem.at[3])
    all_scales = pltpu.make_async_copy(scales_ref, scales, local_sem.at[4])
    for copy in (raw_kv, all_q, own_codes, own_q, all_signs, all_scales):
        copy.start()

    barrier = pltpu.get_barrier_semaphore()

    def greet(target):
        pl.semaphore_signal(barrier, inc=1, device_id={"seq": target}, device_id_type=MESH)

    for k in (2, 3, 1):
        greet(me + off(k))
    greet(me + dy)

    @pl.when(has_up)
    def _():
        greet(up)

    @pl.when(has_down)
    def _():
        greet(down)

    raw_kv.wait()
    pairs = kv_raw[...].reshape(2 * rows, KV * HD)
    to = lax.broadcasted_iota(jnp.int32, (rows, 2 * rows), 0)
    source_row = lax.broadcasted_iota(jnp.int32, (rows, 2 * rows), 1)
    for which in range(2):
        pick = jnp.where(source_row == 2 * to + which, 1.0, 0.0).astype(BF16)
        picked = jnp.dot(pick, pairs, preferred_element_type=F32).astype(BF16)
        for g in range(KV):
            kv_heads[g, :, which * HD:(which + 1) * HD] = picked[:, g * HD:(g + 1) * HD]
    pl.semaphore_wait(barrier, QUAD + has_up.astype(jnp.int32) + has_down.astype(jnp.int32))

    own_kv.start()
    def part_lanes(k):
        return pl.ds((k % 2) * HD, HD)

    def block(slot, k):
        return win.at[slot * QUAD + lane + off(k // 2), :, part_lanes(k)]

    def kv_quad(k):
        return remote(kv_heads.at[lane + off(k // 2), :, part_lanes(k)],
                      win.at[top_slot * QUAD + lane, :, part_lanes(k)],
                      kq_s.at[k], kq_r.at[k], me + off(k // 2))

    def kv_quad_in(k):
        return remote(block(top_slot, k), block(top_slot, k), kq_s.at[k], kq_r.at[k], me + off(k // 2))

    def source(slot, k):
        return kv_heads.at[lane, :, part_lanes(k)] if slot == top_slot and k < 2 else block(slot, k)

    def z_kv(slot, k):
        return remote(source(slot, k), block(slot - 2, k),
                      zs.at[(top_slot - slot) // 2, k], zr.at[(top_slot - slot) // 2, k], up)

    def y_kv(slot, target, k):
        level = (top_slot - 1 - target) // 2
        return remote(source(slot, k), block(target, k), ys.at[level, k], yr.at[level, k], me + dy)

    def there(slot):
        return quad - top_slot + slot >= 0

    def forward_kv(slot, k, act):
        if slot >= 2:
            @pl.when(there(slot) & has_up)
            def _():
                act(z_kv(slot, k))
        if slot >= 1:
            @pl.when(there(slot) & (y == 0))
            def _():
                act(y_kv(slot, slot - 1, k))
        if slot + 1 < top_slot:
            @pl.when(there(slot) & (y == 1))
            def _():
                act(y_kv(slot, slot + 1, k))

    def q_quad(k):
        lanes = pl.ds(pl.multiple_of((lane + off(k)) * width, width), width)
        return remote(q_all.at[:, lanes], qbuf.at[k], qs.at[k], qr.at[k], me + off(k))

    def code_up(k):
        unit = cbuf.at[quad - 2 * k]
        return remote(unit, unit, up_s.at[k + 1], up_r.at[k + 1], up)

    def code_up_in(k):
        unit = cbuf.at[quad - 2 * k]
        return remote(unit, unit, up_s.at[k], up_r.at[k], up)

    def code_down(k):
        unit = cbuf.at[quad + 2 * k]
        return remote(unit, unit, dn_s.at[k + 1], dn_r.at[k + 1], down)

    def code_down_in(k):
        unit = cbuf.at[quad + 2 * k]
        return remote(unit, unit, dn_s.at[k], dn_r.at[k], down)

    half_words = cbuf.shape[1] // 2

    def far(plane):
        return ((plane == 0) | (plane == planes - 1)) & (plane != z)

    def each_y(plane, column, act):
        def copy(unit):
            return remote(unit, unit, cy_s.at[plane], cy_r.at[plane], me + dy)

        @pl.when(far(plane))
        def _():
            act(copy(cbuf.at[plane * 2 + column, pl.ds(0, half_words)]))

        @pl.when(jnp.logical_not(far(plane)))
        def _():
            act(copy(cbuf.at[plane * 2 + column]))

    def send_y(plane):
        each_y(plane, y, lambda copy: copy.start())

    def wait_y(plane):
        each_y(plane, 1 - y, lambda copy: copy.wait_recv())

    def cross_up():
        unit = cbuf.at[1 - y, pl.ds(half_words, half_words)]
        return remote(unit, unit, cross_s.at[0], cross_r.at[0], up)

    def cross_down():
        unit = cbuf.at[(planes - 1) * 2 + 1 - y, pl.ds(half_words, half_words)]
        return remote(unit, unit, cross_s.at[1], cross_r.at[1], down)

    near = jnp.minimum(z, planes - 1 - z)
    toward = jnp.where(z <= planes - 1 - z, 1, -1)

    def plane_at(p):
        both = z + ((p + 1) // 2) * (2 * (p % 2) - 1)
        return jnp.where(p <= 2 * near, both, z + toward * (p - near))

    early = planes + 1

    def relay(p):
        plane = plane_at(p)

        @pl.when(plane < z)
        def _():
            code_up_in(z - plane).wait_recv()

            @pl.when(has_up)
            def _():
                code_up(z - plane).start()
            send_y(plane)

        @pl.when(plane > z)
        def _():
            code_down_in(plane - z).wait_recv()

            @pl.when(has_down)
            def _():
                code_down(plane - z).start()
            send_y(plane)

    def own_y():
        wait_y(z)

        @pl.when((z == 0) & has_up)
        def _():
            cross_up().start()

        @pl.when((z == planes - 1) & has_down)
        def _():
            cross_down().start()

    def relay_cross_up():
        @pl.when(has_down)
        def _():
            cross_up().wait_recv()

            @pl.when(has_up)
            def _():
                cross_up().start()

    def relay_cross_down():
        @pl.when(has_up)
        def _():
            cross_down().wait_recv()

            @pl.when(has_down)
            def _():
                cross_down().start()

    begin = jnp.where(z == 0, 80, jnp.where(z == 1, 138, 165))
    after = jnp.where(z == 0, 295, jnp.where(z == 1, 318, 335))
    stall = 55

    def item_of(q):
        return STEPS + jnp.where(q < early, q, 2 * early + 2 * (q - early))

    events = []

    def expect(action, arrival, deadline, prologue=None):
        step_at = jnp.clip((arrival - begin - 10) // 20, 0, STEPS - 1)
        wait = arrival - after
        later = early + jnp.maximum(wait - 9 * early - stall, 0) // 9
        item_at = STEPS + jnp.where(wait < 9 * early, wait // 9, later)
        at = jnp.minimum(jnp.where(arrival < after, step_at, item_at), deadline)
        if prologue is not None:
            at = jnp.where(prologue, -1, at)
        events.append((action, arrival, at))

    for p in range(1, planes):
        d = plane_at(p) - z
        arrival = jnp.where(d > 0, 130 * d, jnp.where(z == 1, 71, 130) - 117 * d)
        expect(functools.partial(relay, p), arrival, item_of(2 * p - 1), (d == 1) & has_down)
    expect(own_y, jnp.where(z == 0, 185, jnp.where(z == 1, 255, 290)), item_of(1))
    bottom = jnp.where(z == near, 2 * z, planes - 1)
    top_at = jnp.where(planes - 1 - z == near, 2 * near - 1, planes - 1)
    expect(relay_cross_up, jnp.where(z == 1, 275, 170 + 130 * z), item_of(2 * bottom + 1))
    expect(relay_cross_down, 290 + 71 * (planes - 1 - z), item_of(2 * jnp.maximum(top_at, 0) + 1))
    timed = []
    for action, arrival, _ in events:
        at = None
        for _, other_arrival, other_at in events:
            later = jnp.where(other_arrival >= arrival, other_at, STEPS + 4 * planes)
            at = later if at is None else jnp.minimum(at, later)
        timed.append((action, at))

    def run_events(now):
        for action, at in timed:
            pl.when(at == now)(action)

    def score(t, slot, first=0, count=None):
        count = window_blocks if count is None else count
        k = t // HALVES
        half = t % HALVES
        lanes = pl.ds(pl.multiple_of(half * half_width, half_width), half_width)
        q = qbuf[k, :, lanes]
        q = jnp.concatenate([q[:, h * HD:(h + 1) * HD] for h in range(PER_STEP)], axis=0)
        scaled = q.astype(F32) * (LOG2E / math.sqrt(HD))
        high = scaled.astype(BF16)
        low = (scaled - high.astype(F32)).astype(BF16)
        q = jnp.concatenate([high, low], axis=1)
        k_rows = win[pl.ds(lane + off(k) + first, count), :, 0:HD].reshape(count * rows, HD)
        k_rows = jnp.concatenate([k_rows, k_rows], axis=1)
        part = lax.dot_general(q, k_rows, (((1,), (1,)), ((), ())), preferred_element_type=F32)
        sbuf[slot, :, first * rows:(first + count) * rows] = part

    def soft_part(slot, r, first, count):
        scores = sbuf[slot, :, first * rows:(first + count) * rows].reshape(PER_STEP, rows, count * rows)
        head, tail = rows if first == 0 else 0, rows if first + count == window_blocks else 0
        parts = [scores[:, :, head:count * rows - tail]]
        if head:
            parts.insert(0, scores[:, :, :head] + bias[:, :rows][None])
        if tail:
            parts.append(scores[:, :, count * rows - tail:] + bias[:, rows:][None])
        scores = jnp.concatenate(parts, axis=2)
        top = jnp.max(scores, axis=-1, keepdims=True)
        weights = jnp.exp2(scores - top).astype(BF16)
        v_rows = win[pl.ds(r + first, count), :, HD:2 * HD].reshape(count * rows, HD)
        v_rows = jnp.concatenate([v_rows, ones[pl.ds(r + first, count)].reshape(count * rows, HD)], axis=1)
        weighted = jnp.dot(weights.reshape(PER_STEP * rows, count * rows), v_rows, preferred_element_type=F32)
        return top.reshape(PER_STEP * rows, 1), weighted

    def soften(t, slot):
        _, weighted = soft_part(slot, lane + off(t // HALVES), 0, window_blocks)
        wbuf[...] = weighted[:, :HD] / weighted[:, HD:]

    for k in (4, 6, 2, 5, 7, 3):
        kv_quad(k).start()
    for k in (0, 1):
        forward_kv(top_slot, k, lambda copy: copy.start())

    own_codes.wait()

    @pl.when(has_down)
    def _():
        code_down(0).start()
    all_q.wait()
    for k in (1, 2, 3):
        q_quad(k).start()

    for edge, offset in ((0, reach * rows), (1, 0)):
        query = lax.broadcasted_iota(jnp.int32, (rows, rows), 0)
        key = lax.broadcasted_iota(jnp.int32, (rows, rows), 1) - offset
        gap = query - key
        bias[:, edge * rows:(edge + 1) * rows] = jnp.where((gap >= 0) & (gap < WINDOW), 0.0, -jnp.inf).astype(F32)
    for slot in range(slots):
        value = jnp.where(there(slot), 1.0, 0.0).astype(F32)
        ones[slot * QUAD:(slot + 1) * QUAD] = jnp.full((QUAD, rows, HD), value, F32).astype(BF16)

    def take_quad(k):
        kv_quad_in(k).wait_recv()
        forward_kv(top_slot, k, lambda copy: copy.start())

    def take_z(slot, k):
        @pl.when(there(slot))
        def _():
            z_kv(slot + 2, k).wait_recv()
        forward_kv(slot, k, lambda copy: copy.start())

    levels = range(top_slot - 2, -1, -2)
    for k in (2, 3):
        take_quad(k)
    own_kv.wait()
    for k in (0, 1, 2, 3):
        take_z(top_slot - 2, k)
    for k in (4, 6, 5, 7):
        take_quad(k)
    for slot in levels[1:]:
        for k in (0, 1, 2, 3):
            take_z(slot, k)
    for k in (4, 6, 5, 7):
        take_z(top_slot - 2, k)

    for slot in levels[1:]:
        for k in (4, 6, 5, 7):
            take_z(slot, k)

    @pl.when(has_up)
    def _():
        code_up(0).start()

    send_y(z)

    @pl.when(z != 1)
    def _():
        run_events(-1)

    for slot in range(top_slot):
        @pl.when(jnp.logical_not(there(slot)))
        def _():
            first = win[top_slot * QUAD, 0:1, 0:HD].astype(F32)
            fill = jnp.concatenate([jnp.broadcast_to(first, (rows, HD)), jnp.zeros((rows, HD), F32)], axis=1)
            fill = fill.astype(BF16)
            for i in range(QUAD):
                win[slot * QUAD + i] = fill

    late_blocks = 2 * QUAD

    def take_y(slot, pieces):
        for k in pieces:
            @pl.when(there(slot))
            def _():
                level = (top_slot - 1 - slot) // 2
                remote(block(slot, k), block(slot, k), ys.at[level, k], yr.at[level, k], me + dy).wait_recv()

    for slot in range(top_slot - 1, 1, -2):
        take_y(slot, range(2 * QUAD))
    own_q.wait()
    all_signs.wait()
    all_scales.wait()
    score(0, 0, late_blocks, window_blocks - late_blocks)
    near_top, near_sum = soft_part(0, lane, late_blocks, window_blocks - late_blocks)
    tops[...] = jnp.broadcast_to(near_top, tops.shape)
    sums[...] = near_sum

    @pl.when(z == 1)
    def _():
        run_events(-1)
    take_y(1, range(0, 2 * QUAD, 2))
    score(0, 0, 0, late_blocks)
    take_y(1, range(1, 2 * QUAD, 2))
    far_top, far_sum = soft_part(0, lane, 0, late_blocks)
    both_top = jnp.maximum(tops[:, :1], far_top)
    weighted = sums[...] * jnp.exp2(tops[:, :1] - both_top) + far_sum * jnp.exp2(far_top - both_top)
    wbuf[...] = weighted[:, :HD] / weighted[:, HD:]

    def piece(r, source_lane, half):
        start = source_lane * width + half * half_width
        return rot.at[r, :, pl.ds(pl.multiple_of(start, half_width), half_width)]

    def rot_x(t):
        ref = piece(lane + off(t // 2), lane, t % 2)
        return remote(ref, ref, rx_s.at[t], rx_r.at[t], me + dx)

    def rot_c(t):
        ref = piece(lane + off(t // 2), lane, t % 2)
        return remote(ref, ref, rc_s.at[t], rc_r.at[t], me + dc)

    def rot_x_in(t):
        k = t // 2
        ref = piece(lane + dx + (k % 2) * dc - (k // 2) * dx, lane + dx, t % 2)
        return remote(ref, ref, rx_s.at[t], rx_r.at[t], me + dx)

    def rot_f(t):
        k = t // 2
        ref = piece(lane + dx + (k % 2) * dc - (k // 2) * dx, lane + dx, t % 2)
        return remote(ref, ref, rf_s.at[t], rf_r.at[t], me + dc)

    def rot_c_in(t):
        k = t // 2
        ref = piece(lane + dc - (k % 2) * dc + (k // 2) * dx, lane + dc, t % 2)
        return remote(ref, ref, rc_s.at[t], rc_r.at[t], me + dc)

    def rot_f_in(t):
        k = t // 2
        ref = piece(lane + dc + dx - (k % 2) * dc - (k // 2) * dx, lane + dc + dx, t % 2)
        return remote(ref, ref, rf_s.at[t], rf_r.at[t], me + dc)

    def rotate(t):
        k = t // HALVES
        half = t % HALVES
        signs = signs_buf[lane * HALVES + half].astype(F32)
        signed = wbuf[...].reshape(PER_STEP, rows, HD) * signs[:, None, :]
        signed = signed.reshape(PER_STEP * rows, HD)
        high = signed.astype(BF16)
        low = (signed - high.astype(F32)).astype(BF16)
        mixed = jnp.dot(high, had_ref[...], preferred_element_type=F32)
        mixed = mixed + jnp.dot(low, had_ref[...], preferred_element_type=F32)
        mixed = (mixed * (1.0 / math.sqrt(HD))).astype(BF16)
        start = lane * width + half * half_width
        for h in range(PER_STEP):
            rot[lane + off(k), :, pl.ds(pl.multiple_of(start + h * HD, HD), HD)] = mixed[h * rows:(h + 1) * rows]

    def publish(t):
        @pl.when(me < n)
        def _():
            rotate(t)

        @pl.when(t >= LAG)
        def _():
            rot_x_in(t - LAG).wait_recv()
            rot_f(t - LAG).start()

        run_events(t)
        rot_x(t).start()
        rot_c(t).start()

    def step(t, slot):
        score(jnp.minimum(t + 1, STEPS - 1), 1 - slot)
        soften(t, slot)
        publish(t)

    def attend(j, carry):
        k = j + 1
        remote(qbuf.at[k], qbuf.at[k], qs.at[k], qr.at[k], me + off(k)).wait_recv()
        step(2 * j + 1, 1)
        step(2 * j + 2, 0)
        return carry

    publish(jnp.int32(0))
    score(1, 1)
    lax.fori_loop(0, QUAD - 1, attend, 0)
    step(jnp.int32(STEPS - 1), 1)
    for t in range(STEPS - LAG, STEPS // 2):
        rot_x_in(t).wait_recv()
        rot_f(t).start()

    def gathered(t, carry):
        rot_c_in(t).wait_recv()
        return carry

    def gathered_far(t, carry):
        rot_f_in(t).wait_recv()
        return carry

    lax.fori_loop(0, STEPS, gathered, 0)
    lax.fori_loop(0, STEPS // 2, gathered_far, 0)
    chunk_heads = 8
    words = GROUP // 8

    def lanes_of(unit, source_lane):
        s = unit * QUAD + source_lane
        return pl.ds(pl.multiple_of(s * cols, cols), cols)

    def out_send(unit, k):
        target = out_ref.at[:, lanes_of(unit, lane)]
        return remote(stage.at[unit, lane + off(k)], target, os.at[unit, k], orr.at[unit, k], me + off(k))

    def out_recv(unit, k):
        target = out_ref.at[:, lanes_of(unit, lane + off(k))]
        return remote(target, target, os.at[unit, k], orr.at[unit, k], me + off(k))

    def out_own(unit):
        return pltpu.make_async_copy(stage.at[unit, lane], out_ref.at[:, lanes_of(unit, lane)], ol.at[unit])

    def project(unit, side):
        scale = scales[:, lanes_of(unit, lane)]
        acc = jnp.zeros((2 * rows, cols), F32)
        for chunk in range(HEADS // chunk_heads):
            parts = []
            for h in range(chunk * chunk_heads, (chunk + 1) * chunk_heads):
                word = cbuf[unit, h * words:(h + 1) * words, :] ^ jnp.int32(-2004318072)
                factor = jnp.broadcast_to(scale[h:h + 1, :], (words, cols))
                for k in range(8):
                    code = jnp.right_shift(jnp.left_shift(word, 28 - 4 * k), 28)
                    parts.append(code.astype(F32).astype(BF16) * factor)
            weight = jnp.concatenate(parts, axis=0)
            span = chunk_heads * HD
            lhs = rot[pl.ds(2 * side, 2), :, chunk * span:(chunk + 1) * span].reshape(2 * rows, span)
            acc = acc + jnp.dot(lhs, weight, preferred_element_type=F32)
        stage[unit, pl.ds(2 * side, 2)] = acc.astype(BF16).reshape(2, rows, cols)

        @pl.when(side == x)
        def _():
            out_send(unit, 1).start()
            out_own(unit).start()

        @pl.when(side != x)
        def _():
            out_send(unit, 2).start()
            out_send(unit, 3).start()

    def sweep(i, carry):
        first = i < 2 * early
        rest = i - 2 * early
        q = jnp.where(first, i % early, early + rest // 2)
        partner = jnp.where(first, i < early, rest % 2 == 0)
        plane = plane_at(q // 2)
        other = q % 2

        run_events(STEPS + i)

        @pl.when(i == early)
        def _():
            for t in range(max(STEPS - LAG, STEPS // 2), STEPS):
                rot_x_in(t).wait_recv()
                rot_f(t).start()
            lax.fori_loop(STEPS // 2, STEPS, gathered_far, 0)

        @pl.when(partner & (other == 1) & (plane != z))
        def _():
            wait_y(plane)

        project(plane * 2 + y + other * (1 - 2 * y), jnp.where(partner, 1 - x, x))
        return carry

    lax.fori_loop(0, 4 * planes, sweep, 0)

    for k in (1, 2, 3):
        q_quad(k).wait_send()
    for k in range(2, 2 * QUAD):
        kv_quad(k).wait_send()
    for slot in range(top_slot, -1, -2):
        for k in range(2 * QUAD):
            forward_kv(slot, k, lambda copy: copy.wait_send())

    def drain_codes(k, carry):
        @pl.when((z - k >= 0) & has_up)
        def _():
            code_up(k).wait_send()

        @pl.when((z + k < planes) & has_down)
        def _():
            code_down(k).wait_send()
        each_y(k, y, lambda copy: copy.wait_send())
        return carry

    lax.fori_loop(0, planes, drain_codes, 0)

    @pl.when(has_up)
    def _():
        cross_up().wait_send()

    @pl.when(has_down)
    def _():
        cross_down().wait_send()

    def drain_rot(t, carry):
        rot_x(t).wait_send()
        rot_c(t).wait_send()
        rot_f(t).wait_send()
        return carry

    lax.fori_loop(0, STEPS, drain_rot, 0)

    def drain_sent(unit, carry):
        out_own(unit).wait()
        for k in (1, 2, 3):
            out_send(unit, k).wait_send()
        return carry

    lax.fori_loop(0, 2 * planes, drain_sent, 0)

    def drain_out(q, carry):
        unit = plane_at(q // 2) * 2 + y + (q % 2) * (1 - 2 * y)
        for k in (1, 2, 3):
            out_recv(unit, k).wait_recv()
        return carry

    lax.fori_loop(0, 2 * planes, drain_out, 0)


def on_device(queries, keys_values, head_signs, out_codes, out_scales):
    n = lax.axis_size("seq")
    rows = queries.shape[0]
    reach = (WINDOW + rows - 2) // rows
    span = -(-reach // QUAD)
    slots = span + 1
    assert slots % 2 == 1
    planes = n // (2 * QUAD)
    word_rows, cols = out_codes.shape
    vmem = pl.BlockSpec(memory_space=pltpu.VMEM)
    hbm = pl.BlockSpec(memory_space=pltpu.HBM)
    in_hbm = functools.partial(pltpu.with_memory_space_constraint, memory_space=pltpu.HBM)
    dma = pltpu.SemaphoreType.DMA
    return pl.pallas_call(
        functools.partial(kernel, n, reach, slots),
        out_shape=pltpu.VMEM((rows, n * cols), BF16),
        in_specs=[hbm, hbm, hbm, vmem, hbm, hbm],
        out_specs=pl.BlockSpec(memory_space=pl.ANY),
        scratch_shapes=[
            pltpu.VMEM((slots * QUAD, rows, 2 * HD), BF16),
            pltpu.VMEM((slots * QUAD, rows, HD), BF16),
            pltpu.VMEM((QUAD, rows, LANE_HEADS * HD), BF16),
            pltpu.VMEM((2 * planes, word_rows, cols), jnp.int32),
            pltpu.VMEM((QUAD, rows, HEADS * HD), BF16),
            pltpu.VMEM((rows, 2 * rows), F32),
            pltpu.VMEM((2, PER_STEP * rows, (reach + 1) * rows), F32),
            pltpu.VMEM((PER_STEP * rows, HD), F32),
            pltpu.VMEM((PER_STEP * rows, HD), F32),
            pltpu.VMEM((PER_STEP * rows, 2 * HD), F32),
            pltpu.VMEM((2 * planes, QUAD, rows, cols), BF16),
            pltpu.VMEM((rows, HEADS * HD), BF16),
            pltpu.VMEM((STEPS, PER_STEP, HD), jnp.int32),
            pltpu.VMEM((HEADS, n * cols), BF16),
            pltpu.VMEM((rows, 2, KV * HD), BF16),
            pltpu.VMEM((KV, rows, 2 * HD), BF16),
            dma((7,)),
            dma((2 * QUAD,)), dma((2 * QUAD,)),
            dma((QUAD,)), dma((QUAD,)),
            dma((slots // 2, 2 * QUAD)), dma((slots // 2, 2 * QUAD)),
            dma((slots // 2, 2 * QUAD)), dma((slots // 2, 2 * QUAD)),
            dma((planes + 1,)), dma((planes + 1,)),
            dma((planes + 1,)), dma((planes + 1,)),
            dma((planes,)), dma((planes,)),
            dma((2,)), dma((2,)),
            dma((STEPS,)), dma((STEPS,)),
            dma((STEPS,)), dma((STEPS,)),
            dma((STEPS,)), dma((STEPS,)),
            dma((2 * planes, QUAD)), dma((2 * planes, QUAD)),
            dma((2 * planes,)),
        ],
        compiler_params=pltpu.CompilerParams(
            collective_id=0, has_side_effects=True, vmem_limit_bytes=52 * 1000 * 1000
        ),
    )(
        in_hbm(queries),
        in_hbm(keys_values),
        in_hbm(head_signs.reshape(STEPS, PER_STEP, HD)),
        reordered_hadamard(),
        in_hbm(out_codes),
        in_hbm(out_scales),
    )


def solution(mesh):
    return jax.shard_map(
        on_device,
        mesh=mesh,
        in_specs=(
            P(("groups", "seq"), None),
            P(("groups", "seq"), None, None),
            P(),
            P(None, "seq"),
            P(),
        ),
        out_specs=P(("groups", "seq"), None),
        check_vma=False,
    )
```
